256 devices in a mesh: rep: 4 (over z_hi), own: 64 (over x, z_lo, y, core).
Axes of the slice: x: 4, y: 4, z: 8 (z_hi: 4, z_lo: 2; z = z_hi * 2 + z_lo), core: 2. Of those that a mesh axis runs over, the one named last changes fastest.
Arguments:
- inputs: bfloat16 [65536, 8192], P(('rep', 'own')), may hold values from -24 to 24
- cotangent: bfloat16 [65536, 8192], P(('rep', 'own')), may hold values from -6 to 6
- gate: float32 [65536], P(('rep', 'own')), may hold values from 0.05 to 0.95
- down_weight: bfloat16 [8192, 256], P('rep'), may hold values from -0.0625 to 0.0625
- up_weight: bfloat16 [8192, 256], P('rep'), may hold values from -0.0625 to 0.0625
- mixing: bfloat16 [256, 256], replicated, may hold values from -0.375 to 0.375
- owner_table: int32 [64, 1], replicated, may hold values from -1 to 31, as said below
- left_factor: float32 [64, 256, 256], P('own'), as said below
- right_factor: float32 [64, 256, 256], P('own'), as said below
Outputs:
- preconditioned: float32 [16384, 256], P('own')
The draws below stay inside these ranges and needn't reach their ends.
Inputs may be any that keep to these rules, and one draw needn't show every extreme that they name: `owner_table`: each of the 32 block ids stands in exactly one slot; -1 marks an empty slot; some owner has all 1 slots filled. `left_factor`: every slot's matrix is symmetric positive definite. `right_factor`: every slot's matrix is symmetric positive definite.
All inputs are finite; a program needn't handle non-finite values.
Results may differ from the reference program's by a relative error of at most 0.0077.
Values may be sent and summed in bfloat16 or wider, within the bound.
A program may use at most 128 MiB of HBM per device.

```python
import jax
import jax.numpy as jnp
from jax import lax

D = 8192
R = 256
ITERS = 5
B_DEV = 256
TOKENS = 65536
NBLK = 32
MOST = 1
N_OWN = 64


def draw_owner_table(key, part):
    slot_total = N_OWN * MOST
    first_key, second_key, third_key = jax.random.split(jax.random.fold_in(key, 7), 3)
    filled_owner = jax.random.randint(first_key, (), 0, N_OWN)
    shuffled = jax.random.permutation(second_key, slot_total).astype(jnp.int32)
    owner_ids = jnp.arange(slot_total, dtype=jnp.int32) // MOST
    priority = shuffled - slot_total * (owner_ids == filled_owner).astype(jnp.int32)
    ranked = jnp.argsort(priority, stable=True)
    block_order = jax.random.permutation(third_key, NBLK).astype(jnp.int32)
    contents = jnp.concatenate([block_order, jnp.full((slot_total - NBLK,), -1, jnp.int32)])
    assigned = jnp.zeros((slot_total,), jnp.int32).at[ranked].set(contents)
    return assigned.reshape(N_OWN, MOST)


def spd_factor(key):
    slot_total = N_OWN * MOST
    base_key = jax.random.fold_in(key, 0)
    samples = jax.random.normal(base_key, (slot_total, R, 2 * R), jnp.float32)
    gram = jnp.einsum('kij,klj->kil', samples, samples, precision=lax.Precision.HIGHEST)
    return gram * (0.01 / (2.0 * TOKENS))


def draw_left_factor(key, part):
    return spd_factor(jax.random.fold_in(key, 11))


def draw_right_factor(key, part):
    return spd_factor(jax.random.fold_in(key, 12))


def raised(entries, own_key, source, target, parts, factor):
    owner, partner = [(jnp.arange(entries.shape[axis_at]) // (entries.shape[axis_at] // parts)).reshape([-1 if axis == axis_at else 1 for axis in range(entries.ndim)]) for axis_at in (source, target)]
    chosen = jax.random.permutation(own_key, parts)[partner]
    strong = (owner == chosen) | (owner == (partner + parts // 2) % parts)
    return jnp.where(strong, factor * entries, entries)


def level_of(own_key, dims, cuts, least, high):
    loudness, own = 1.0, jax.random.fold_in(own_key, 6)
    for dim, parts in cuts:
        heights = jnp.exp(jax.random.uniform(jax.random.fold_in(own, dim), (parts,), jnp.float32, least / len(cuts), high / len(cuts)))
        loudness = loudness * jnp.repeat(heights, dims[dim] // parts).reshape([-1 if axis == dim else 1 for axis in range(len(dims))])
    return loudness


def noise(stream_key, shape, spread, most, cuts=(), kind=jnp.bfloat16):
    drawn = jax.random.normal(stream_key, shape, jnp.float32) * spread
    if len(cuts) > 0:
        drawn = level_of(stream_key, shape, cuts, -0.22, 0.18) * drawn
    return jnp.clip(drawn, min=-most, max=most).astype(kind)


def noise_with(own_key, dims, deviation, limit, cuts, heavy, kind=jnp.bfloat16):
    values = deviation * jax.random.normal(own_key, dims, jnp.float32)
    if cuts:
        values = values * level_of(own_key, dims, cuts, -0.22, 0.18)
    return jnp.clip(raised(values, jax.random.fold_in(own_key, 3), *heavy), -limit, limit).astype(kind)


def setup_inputs(seed: int = 0) -> dict:
    seeds = jax.random.split(jax.random.key(seed), 10)
    return {
        "inputs": noise_with(seeds[0], (TOKENS, D), 1.0, 24.0, ((0, 256),), (0, 1, 256, 6.0)),
        "cotangent": noise(seeds[1], (TOKENS, D), 1.0, 6.0, ((0, 256),)),
        "gate": jnp.clip(0.05 + 0.9 * jax.random.uniform(seeds[2], (TOKENS,), jnp.float32) ** level_of(seeds[2], (TOKENS,), ((0, 256),), -0.2, 0.2), 0.05, 0.95),
        "down_weight": noise(seeds[3], (D, R), D ** -0.5, 0.0625, ((0, 4),)),
        "up_weight": noise(seeds[4], (D, R), D ** -0.5, 0.0625, ((0, 4),)),
        "mixing": noise(seeds[5], (R, R), R ** -0.5, 0.375),
        "owner_table": draw_owner_table(jax.random.fold_in(seeds[9], 71), 0),
        "left_factor": draw_left_factor(jax.random.fold_in(seeds[9], 71), 0),
        "right_factor": draw_right_factor(jax.random.fold_in(seeds[9], 71), 0),
    }


BETA = 0.95
EPS = 1e-06

def batched(left, right):
    return jnp.einsum('kij,kjl->kil', left, right, precision=lax.Precision.HIGHEST)

def inverse_root(matrices):
    width = matrices.shape[-1]
    identity = jnp.eye(width, dtype=jnp.float32)
    shifted = matrices + EPS * identity
    norm_size = jnp.sqrt(lax.optimization_barrier(jnp.sum(shifted * shifted, axis=(1, 2))))
    result = jnp.broadcast_to(identity, shifted.shape) * (norm_size ** (-0.25))[:, None, None]
    normed = shifted / norm_size[:, None, None]
    for sweep in range(ITERS):
        factor = (5.0 * identity - normed) / 4.0
        result = batched(result, factor)
        square = batched(factor, factor)
        normed = batched(batched(square, square), normed)
    return result

def backward_signal(rows, tangent, gate_rows, down_weight, up_weight, mixing):
    lifted = (gate_rows[:, None] * rows.astype(jnp.float32) * tangent.astype(jnp.float32)).astype(jnp.bfloat16)
    projected = jnp.dot(rows, down_weight, preferred_element_type=jnp.float32)
    back_proj = jnp.dot(lifted, up_weight, preferred_element_type=jnp.float32)
    inner_act = jnp.tanh(projected).astype(jnp.bfloat16)
    outer_act = jnp.tanh(jnp.dot(inner_act, mixing, preferred_element_type=jnp.float32))
    outer_slope = (back_proj * (1.0 - outer_act * outer_act)).astype(jnp.bfloat16)
    through = lax.dot_general(outer_slope, mixing, (((1,), (1,)), ((), ())), preferred_element_type=jnp.float32)
    inner_wide = inner_act.astype(jnp.float32)
    return (through * (1.0 - inner_wide * inner_wide)).astype(jnp.bfloat16)

def reference(inputs, cotangent, gate, down_weight, up_weight, mixing, owner_table, left_factor, right_factor):
    group_count = inputs.shape[0] // B_DEV

    def accumulate(summed, minibatch):
        rows, tangent, gate_rows = minibatch
        signal = backward_signal(rows, tangent, gate_rows, down_weight, up_weight, mixing)
        return (summed + lax.dot_general(rows, signal, (((0,), (0,)), ((), ())), preferred_element_type=jnp.float32), None)
    start_sum = jnp.zeros((D, R), jnp.float32)
    gradient, _ = lax.scan(accumulate, start_sum, (inputs.reshape(group_count, B_DEV, D), cotangent.reshape(group_count, B_DEV, D), gate.reshape(group_count, B_DEV)))
    gradient = gradient / TOKENS
    table_flat = owner_table.reshape(-1)
    filled_slots = (table_flat >= 0)[:, None, None]
    blocks = gradient.reshape(NBLK, R, R)
    gradients = jnp.where(filled_slots, blocks[jnp.maximum(table_flat, 0).astype(jnp.int32)], 0.0)
    flipped = jnp.swapaxes(gradients, 1, 2)
    left_new = BETA * left_factor + (1.0 - BETA) * batched(gradients, flipped)
    right_new = BETA * right_factor + (1.0 - BETA) * batched(flipped, gradients)
    slot_total = N_OWN * MOST
    left_root = inverse_root(left_new)
    right_root = inverse_root(right_new)
    preconditioned = batched(batched(left_root, gradients), right_root)
    return jnp.where(filled_slots, preconditioned, 0.0).reshape(slot_total * R, R)
```

```python
import functools

import jax
import jax.numpy as jnp
from jax import lax
from jax.experimental import pallas as pl
from jax.experimental.pallas import tpu as pltpu
from jax.sharding import PartitionSpec as P

R = 256
ITERS = 5
BETA = 0.95
EPS = 1e-06
TOKENS = 65536

F32 = jnp.float32
BF16 = jnp.bfloat16
MESH = pl.DeviceIdType.MESH


def own_of(x, zl, y, c):
    return ((x * 2 + zl) * 4 + y) * 2 + c


def reduce_kernel(
    x_hbm, cot_hbm, gate_ref, down_hbm, up_hbm, mix_ref, table_ref, out_ref,
    wbuf, xv, lv, gcol, pacc, sigp, dsend, drecv, acc,
    s1send, s1rel, s1recv, s2f, s2send, s2recv, zf, zsend, zrecv, zag, stage, arecv,
    ld, wsend, w1r, st1r, st2r, ddr, gsend, gdr, s1relr, s1r, s2r, zr, zagr, asend, ar,
):
    r = lax.axis_index("rep")
    o = lax.axis_index("own")
    c = lax.rem(o, 2)
    y = lax.rem(o // 2, 4)
    zl = lax.rem(o // 8, 2)
    x = o // 16
    z = r * 2 + zl
    m = (x * 4 + y) * 2 + c
    sgn = 2 * zl - 1
    partner = (r, own_of(x, zl, y, 1 - c))

    def along(axis, d):
        if axis == 0:
            return (r, own_of(lax.rem(x + d + 4, 4), zl, y, c))
        return (r, own_of(x, zl, lax.rem(y + d + 4, 4), c))

    def zpeer(d):
        zz = lax.rem(z + d + 8, 8)
        return (zz // 2, own_of(x, lax.rem(zz, 2), y, c))

    def plane(mm):
        return (r, own_of(mm // 8, zl, lax.rem(mm // 2, 4), lax.rem(mm, 2)))

    quarter = [r, lax.rem(r + sgn + 4, 4), lax.rem(r - sgn + 4, 4), lax.rem(r + 2, 4)]

    pending = []

    def send(src, dst, ssem, rsem, dev):
        cp = pltpu.make_async_remote_copy(
            src_ref=src, dst_ref=dst, send_sem=ssem, recv_sem=rsem,
            device_id=dev, device_id_type=MESH,
        )
        cp.start()
        pending.append(cp)

    def arrived(dst, rsem, dev):
        pltpu.make_async_remote_copy(
            src_ref=dst, dst_ref=dst, send_sem=rsem, recv_sem=rsem,
            device_id=dev, device_id_type=MESH,
        ).wait_recv()

    loads = [
        pltpu.make_async_copy(down_hbm, wbuf.at[0, 0], ld.at[0]),
        pltpu.make_async_copy(up_hbm, wbuf.at[0, 1], ld.at[1]),
    ]
    for s in range(4):
        cols = pl.ds(pl.multiple_of(quarter[s] * 2048, 2048), 2048)
        loads.append(pltpu.make_async_copy(x_hbm.at[:, cols], xv.at[:, cols], ld.at[2 + 2 * s]))
        loads.append(pltpu.make_async_copy(cot_hbm.at[:, cols], lv.at[:, cols], ld.at[3 + 2 * s]))
    for cp in loads:
        cp.start()

    barrier = pltpu.get_barrier_semaphore()

    def greet_z(d, carry):
        pl.semaphore_signal(barrier, inc=1, device_id=zpeer(d), device_id_type=MESH)
        return carry

    def greet_p(e, carry):
        pl.semaphore_signal(
            barrier, inc=1, device_id=plane(lax.rem(m + e, 32)), device_id_type=MESH
        )
        return carry

    lax.fori_loop(1, 8, greet_z, 0)
    lax.fori_loop(1, 32, greet_p, 0)
    pl.semaphore_wait(barrier, 38)

    pos = (x, y)
    nws = [0]

    def wsem():
        nws[0] += 1
        return wsend.at[nws[0] - 1]

    def base(cc, k):
        return cc * 1024 + k * 512

    def piece(slot, k, p1, p2):
        rows = pl.ds(pl.multiple_of(base(c, k) + (p2 * 4 + p1) * 32, 32), 32)
        return rows

    def group(slot, k, p2):
        return pl.ds(pl.multiple_of(base(c, k) + p2 * 128, 128), 128)

    def p12(k):
        return (pos[0], pos[1]) if k == 0 else (pos[1], pos[0])

    def near(p, d):
        return lax.rem(p + d + 4, 4)

    loads[0].wait()
    loads[1].wait()
    zdest = [
        (lax.rem(r + sgn + 4, 4), own_of(x, 1 - zl, y, c)),
        (lax.rem(r + sgn + 4, 4), own_of(x, zl, y, c)),
        (lax.rem(r + 2, 4), own_of(x, 1 - zl, y, c)),
    ]
    for s in range(1, 4):
        for k in range(2):
            rows = piece(0, k, *p12(k))
            send(
                wbuf.at[0, :, rows, :], wbuf.at[s, :, rows, :],
                wsem(), w1r.at[s - 1, k], zdest[s - 1],
            )

    def stage_direct(s, k, stg):
        p1, p2 = p12(k)
        axis = k if stg == 1 else 1 - k
        rows = piece(s, k, p1, p2) if stg == 1 else group(s, k, p2)
        sems = st1r if stg == 1 else st2r
        send(wbuf.at[s, :, rows, :], wbuf.at[s, :, rows, :], wsem(), sems.at[s - 1, k, 0], along(axis, 1))
        send(wbuf.at[s, :, rows, :], wbuf.at[s, :, rows, :], wsem(), sems.at[s - 1, k, 1], along(axis, -1))

    def rows_at(s, k, stg, d):
        p1, p2 = p12(k)
        return piece(s, k, near(p1, d), p2) if stg == 1 else group(s, k, near(p2, d))

    def stage_forward(s, k, stg):
        axis = k if stg == 1 else 1 - k
        sems = st1r if stg == 1 else st2r
        rm = rows_at(s, k, stg, -1)
        rp = rows_at(s, k, stg, 1)
        arrived(wbuf.at[s, :, rm, :], sems.at[s - 1, k, 0], along(axis, -1))
        send(wbuf.at[s, 0, rm, :], wbuf.at[s, 0, rm, :], wsem(), sems.at[s - 1, k, 2], along(axis, 1))
        arrived(wbuf.at[s, :, rp, :], sems.at[s - 1, k, 1], along(axis, 1))
        send(wbuf.at[s, 1, rp, :], wbuf.at[s, 1, rp, :], wsem(), sems.at[s - 1, k, 3], along(axis, -1))

    def stage_far(s, k, stg):
        axis = k if stg == 1 else 1 - k
        sems = st1r if stg == 1 else st2r
        rf = rows_at(s, k, stg, 2)
        arrived(wbuf.at[s, 0, rf, :], sems.at[s - 1, k, 2], along(axis, -1))
        arrived(wbuf.at[s, 1, rf, :], sems.at[s - 1, k, 3], along(axis, 1))

    def s1(s):
        for k in range(2):
            arrived(wbuf.at[s, :, piece(s, k, *p12(k)), :], w1r.at[s - 1, k], zpeer(1))
            stage_direct(s, k, 1)

    def f1(s):
        for k in range(2):
            stage_forward(s, k, 1)

    def s2(s):
        for k in range(2):
            stage_far(s, k, 1)
            stage_direct(s, k, 2)

    def f2(s):
        for k in range(2):
            stage_forward(s, k, 2)

    def d2d(s):
        for k in range(2):
            stage_far(s, k, 2)
            rows = pl.ds(pl.multiple_of(base(c, k), 512), 512)
            send(wbuf.at[s, :, rows, :], wbuf.at[s, :, rows, :], wsem(), ddr.at[s - 1, k], partner)

    def lift(s):
        loads[2 + 2 * s].wait()
        loads[3 + 2 * s].wait()

        def body(i, carry):
            cols = pl.ds(pl.multiple_of(quarter[s] * 2048 + i * 128, 128), 128)
            g = gcol[...]
            lv[:, cols] = (g * xv[:, cols].astype(F32) * lv[:, cols].astype(F32)).astype(BF16)
            return carry

        lax.fori_loop(0, 16, body, 0)

    def matmul(s, cc):
        rows = pl.ds(pl.multiple_of(cc * 1024, 1024), 1024)
        cols = pl.ds(pl.multiple_of(quarter[s] * 2048 + cc * 1024, 1024), 1024)
        pacc[0] += jnp.dot(xv[:, cols], wbuf[s, 0, rows, :], preferred_element_type=F32)
        pacc[1] += jnp.dot(lv[:, cols], wbuf[s, 1, rows, :], preferred_element_type=F32)

    gcol[...] = jnp.transpose(jnp.broadcast_to(gate_ref[...], (128, 256)))
    pacc[...] = jnp.zeros_like(pacc)
    s1(1)
    lift(0)
    s1(2)
    f1(1)
    lift(1)
    s1(3)
    f1(2)
    s2(1)
    matmul(0, c)
    f1(3)
    s2(2)
    matmul(0, 1 - c)
    f2(1)
    s2(3)
    lift(2)
    f2(2)
    d2d(1)
    lift(3)
    f2(3)
    matmul(1, c)
    d2d(2)
    matmul(2, c)

    def from_partner(s):
        for k in range(2):
            rows = pl.ds(pl.multiple_of(base(1 - c, k), 512), 512)
            arrived(wbuf.at[s, :, rows, :], ddr.at[s - 1, k], partner)
        matmul(s, 1 - c)

    from_partner(1)
    from_partner(2)
    d2d(3)
    matmul(3, c)
    from_partner(3)

    inner = jnp.tanh(pacc[0]).astype(BF16)
    outer = jnp.tanh(jnp.dot(inner, mix_ref[...], preferred_element_type=F32))
    slope = (pacc[1] * (1.0 - outer * outer)).astype(BF16)
    through = lax.dot_general(
        slope, mix_ref[...], (((1,), (1,)), ((), ())), preferred_element_type=F32
    )
    inner_wide = inner.astype(F32)
    signal = through * (1.0 - inner_wide * inner_wide)
    sigp[...] = jnp.transpose(signal).astype(BF16)
    other_rows = pl.ds(pl.multiple_of((1 - c) * 128, 128), 128)
    own_rows = pl.ds(pl.multiple_of(c * 128, 128), 128)

    ngs = [0]

    def gsem():
        ngs[0] += 1
        return gsend.at[ngs[0] - 1]

    for g in range(4):

        def grad(i, carry, g=g):
            b = g * 8 + i
            cols = pl.ds(pl.multiple_of(b * 256, 256), 256)
            xb = xv[:, cols]
            dsend[b] = jnp.dot(sigp[other_rows, :], xb, preferred_element_type=F32).astype(BF16)
            acc[b] = jnp.dot(sigp[own_rows, :], xb, preferred_element_type=F32)
            return carry

        lax.fori_loop(0, 8, grad, 0)
        blk = pl.ds(g * 8, 8)
        send(dsend.at[blk], drecv.at[blk], gsem(), gdr.at[g], partner)

    def rows16(k, d):
        i = near(pos[k], d)
        return pl.ds(pl.multiple_of(k * 64 + i * 16, 16), 16)

    for g in range(4):
        blk = pl.ds(g * 8, 8)
        arrived(drecv.at[blk], gdr.at[g], partner)

        def merge(i, carry, g=g):
            b = g * 8 + i
            acc[b] = acc[b] + drecv[b].astype(F32)
            for k in range(2):
                s1send[k, 0, b] = acc[b, rows16(k, 2), :].astype(BF16)
                d = 1 if g >= 2 else -1
                s1send[k, 1 if g >= 2 else 2, b] = acc[b, rows16(k, d), :].astype(BF16)
            return carry

        lax.fori_loop(0, 8, merge, 0)
        for k in range(2):
            if g < 2:
                send(s1send.at[k, 0, blk], s1rel.at[k, 0, blk], gsem(), s1relr.at[k, 0, g], along(k, 1))
                send(s1send.at[k, 2, blk], s1recv.at[k, 1, blk], gsem(), s1r.at[k, 1, g], along(k, -1))
            else:
                rel = pl.ds((g - 2) * 8, 8)
                send(s1send.at[k, 0, blk], s1rel.at[k, 1, rel], gsem(), s1relr.at[k, 1, g - 2], along(k, -1))
                send(s1send.at[k, 1, blk], s1recv.at[k, 0, blk], gsem(), s1r.at[k, 0, g], along(k, 1))

    for side in range(2):
        for h in range(2):
            g = 2 * side + h
            for k in range(2):
                blk = pl.ds(g * 8, 8)
                rel = pl.ds(h * 8, 8)
                d = 1 if side == 0 else -1
                arrived(s1rel.at[k, side, rel], s1relr.at[k, side, h], along(k, -d))

                def relay(i, carry, g=g, h=h, k=k, side=side, d=d):
                    b = g * 8 + i
                    s1send[k, 1 + side, b] = (
                        acc[b, rows16(k, d), :] + s1rel[k, side, h * 8 + i].astype(F32)
                    ).astype(BF16)
                    return carry

                lax.fori_loop(0, 8, relay, 0)
                send(s1send.at[k, 1 + side, blk], s1recv.at[k, side, blk], gsem(), s1r.at[k, side, g], along(k, d))

    for k in range(2):
        for g in (2, 3):
            arrived(s1recv.at[k, 0, pl.ds(g * 8, 8)], s1r.at[k, 0, g], along(k, -1))
        for g in (0, 1):
            arrived(s1recv.at[k, 1, pl.ds(g * 8, 8)], s1r.at[k, 1, g], along(k, 1))
    for k in range(2):
        for g in (0, 1):
            arrived(s1recv.at[k, 0, pl.ds(g * 8, 8)], s1r.at[k, 0, g], along(k, -1))
        for g in (2, 3):
            arrived(s1recv.at[k, 1, pl.ds(g * 8, 8)], s1r.at[k, 1, g], along(k, 1))

        def own_sum(i, carry, k=k):
            tot = []
            for q in range(2):
                b = i * 2 + q
                tot.append(
                    acc[b, rows16(k, 0), :]
                    + s1recv[k, 0, b].astype(F32)
                    + s1recv[k, 1, b].astype(F32)
                )
            rows = pl.ds(pl.multiple_of(i * 16, 16), 16)
            for j in range(4):
                a, h = j // 2, j % 2
                part = jnp.concatenate(
                    [t[a * 8 : a * 8 + 8, h * 128 : h * 128 + 128] for t in tot], axis=0
                )
                s2f[k, j, rows, :] = part
                s2send[k, j, rows, :] = part.astype(BF16)
            return carry

        lax.fori_loop(0, 16, own_sum, 0)
        for d in (1, 3, 2):
            j = near(pos[1 - k], d)
            send(s2send.at[k, j], s2recv.at[k, d - 1], gsem(), s2r.at[k, d - 1], along(1 - k, d))

    parts = []
    for k in range(2):
        tot = s2f[k, pos[1 - k]]
        for d in (1, 3, 2):
            arrived(s2recv.at[k, d - 1], s2r.at[k, d - 1], along(1 - k, -d))
            tot = tot + s2recv[k, d - 1].astype(F32)
        parts.append(tot.reshape(32, 8, 128))
    both = jnp.concatenate(parts, axis=1)
    zf[...] = both
    zsend[...] = both.astype(BF16)

    for d in (4, 3, 5, 2, 6, 1, 7):
        zz = lax.rem(z + d, 8)
        send(zsend.at[pl.ds(zz * 4, 4)], zrecv.at[d - 1], gsem(), zr.at[d - 1], zpeer(d))
    tot = zf[pl.ds(z * 4, 4)]
    for d in (1, 7, 2, 6, 3, 5, 4):
        arrived(zrecv.at[d - 1], zr.at[d - 1], zpeer(-d))
        tot = tot + zrecv[d - 1].astype(F32)
    mine = pl.ds(z * 4, 4)
    zag[mine] = tot.astype(BF16)
    for d in (4, 3, 5, 2, 6, 1, 7):
        send(zag.at[mine], zag.at[mine], gsem(), zagr.at[d - 1], zpeer(d))
    for d in (1, 7, 2, 6, 3, 5, 4):
        zz = lax.rem(z - d + 8, 8)
        arrived(zag.at[pl.ds(zz * 4, 4)], zagr.at[d - 1], zpeer(-d))

    def choose(mm, carry):
        _, oo = plane(mm)
        stage[mm] = zag[jnp.maximum(table_ref[oo], 0)]
        return carry

    lax.fori_loop(0, 32, choose, 0)

    def to_owner(e):
        mm = lax.rem(m + e, 32)
        return pltpu.make_async_remote_copy(
            src_ref=stage.at[mm], dst_ref=arecv.at[m], send_sem=asend.at[e - 1],
            recv_sem=ar.at[e - 1], device_id=plane(mm), device_id_type=MESH,
        )

    def go(e, carry):
        to_owner(e).start()
        return carry

    lax.fori_loop(1, 32, go, 0)
    arecv[m] = stage[m]

    def land(e, carry):
        mm = lax.rem(m - e + 32, 32)
        arrived(arecv.at[mm], ar.at[e - 1], plane(mm))
        return carry

    lax.fori_loop(1, 32, land, 0)
    for xx in range(4):
        for yy in range(4):
            for cc in range(2):
                tile = arecv[(xx * 4 + yy) * 2 + cc].astype(F32)
                r0 = cc * 128 + xx * 16 + (yy // 2) * 8
                l0 = (yy % 2) * 128
                out_ref[r0 : r0 + 8, l0 : l0 + 128] = tile[0:8]
                r1 = cc * 128 + 64 + yy * 16 + (xx // 2) * 8
                l1 = (xx % 2) * 128
                out_ref[r1 : r1 + 8, l1 : l1 + 128] = tile[8:16]

    def drain(e, carry):
        to_owner(e).wait_send()
        return carry

    lax.fori_loop(1, 32, drain, 0)
    for cp in pending:
        cp.wait_send()


def reduced_block(inputs, cotangent, gate, down_weight, up_weight, mixing, table):
    any_spec = pl.BlockSpec(memory_space=pl.ANY)
    vm = pl.BlockSpec(memory_space=pltpu.VMEM)
    dma = pltpu.SemaphoreType.DMA
    V = pltpu.VMEM
    return pl.pallas_call(
        reduce_kernel,
        name="reduce",
        out_shape=jax.ShapeDtypeStruct((256, 256), F32),
        in_specs=[any_spec, any_spec, vm, any_spec, any_spec, vm,
                  pl.BlockSpec(memory_space=pltpu.SMEM)],
        out_specs=vm,
        scratch_shapes=[
            V((4, 2, 2048, 256), BF16),
            V((256, 8192), BF16),
            V((256, 8192), BF16),
            V((256, 128), F32),
            V((2, 256, 256), F32),
            V((256, 256), BF16),
            V((32, 128, 256), BF16),
            V((32, 128, 256), BF16),
            V((32, 128, 256), F32),
            V((2, 3, 32, 16, 256), BF16),
            V((2, 2, 16, 16, 256), BF16),
            V((2, 2, 32, 16, 256), BF16),
            V((2, 4, 256, 128), F32),
            V((2, 4, 256, 128), BF16),
            V((2, 3, 256, 128), BF16),
            V((32, 16, 128), F32),
            V((32, 16, 128), BF16),
            V((7, 4, 16, 128), BF16),
            V((32, 16, 128), BF16),
            V((32, 16, 128), BF16),
            V((32, 16, 128), BF16),
            dma((10,)),
            dma((60,)),
            dma((3, 2)),
            dma((3, 2, 4)),
            dma((3, 2, 4)),
            dma((3, 2)),
            dma((48,)),
            dma((4,)),
            dma((2, 2, 2)),
            dma((2, 2, 4)),
            dma((2, 3)),
            dma((7,)),
            dma((7,)),
            dma((31,)),
            dma((31,)),
        ],
        compiler_params=pltpu.CompilerParams(
            collective_id=0, has_side_effects=True, vmem_limit_bytes=56 * 1024 * 1024
        ),
    )(inputs, cotangent, gate, down_weight, up_weight, mixing, table)


def halves(a):
    hi = a.astype(BF16)
    return hi, (a - hi.astype(F32)).astype(BF16)


def product(a, b):
    (ah, al), (bh, bl) = a, b
    lhs = jnp.concatenate([ah, ah, al], axis=1)
    rhs = jnp.concatenate([bh, bl, bh], axis=0)
    return jnp.dot(lhs, rhs, preferred_element_type=F32)


def root_kernel(gt_ref, left_ref, right_ref, table_ref, out_ref):
    eye = (
        lax.broadcasted_iota(jnp.int32, (R, R), 0) == lax.broadcasted_iota(jnp.int32, (R, R), 1)
    ).astype(F32)
    gt = gt_ref[...] * (1.0 / TOKENS)
    gs = halves(jnp.transpose(gt))
    gts = halves(gt)
    news = [
        BETA * left_ref[0] + (1.0 - BETA) * product(gs, gts),
        BETA * right_ref[0] + (1.0 - BETA) * product(gts, gs),
    ]
    results, norms = [], []
    for a in news:
        shifted = a + EPS * eye
        total = jnp.sum(shifted * shifted, keepdims=True)
        norm = jnp.sqrt(total)
        results.append(lax.rsqrt(jnp.sqrt(norm)))
        norms.append(shifted / norm)
    for sweep in range(ITERS):
        for i in range(2):
            factor = (5.0 * eye - norms[i]) / 4.0
            fs = halves(factor)
            if sweep == 0:
                results[i] = results[i] * factor
            else:
                results[i] = product(halves(results[i]), fs)
            if sweep < ITERS - 1:
                ss = halves(product(fs, fs))
                ms = halves(norms[i])
                norms[i] = product(halves(product(ss, ss)), ms)
    done = product(halves(product(halves(results[0]), gs)), halves(results[1]))
    filled = table_ref[lax.axis_index("own")] >= 0
    out_ref[...] = jnp.where(filled, done, 0.0)


def preconditioned(gt, left, right, table):
    vm = pl.BlockSpec(memory_space=pltpu.VMEM)
    return pl.pallas_call(
        root_kernel,
        name="roots",
        out_shape=jax.ShapeDtypeStruct((R, R), F32),
        in_specs=[vm, vm, vm, pl.BlockSpec(memory_space=pltpu.SMEM)],
        out_specs=vm,
    )(gt, left, right, table)


def shards(
    inputs, cotangent, gate, down_weight, up_weight, mixing, owner_table, left_factor, right_factor
):
    table = owner_table.reshape(-1)
    gt = reduced_block(
        inputs, cotangent, gate.reshape(1, -1), down_weight, up_weight, mixing, table
    )
    return preconditioned(gt, left_factor, right_factor, table)


def solution(mesh):
    in_specs = (
        P(("rep", "own"), None),
        P(("rep", "own"), None),
        P(("rep", "own")),
        P("rep", None),
        P("rep", None),
        P(),
        P(),
        P("own", None, None),
        P("own", None, None),
    )
    return jax.shard_map(
        shards, mesh=mesh, in_specs=in_specs, out_specs=P("own", None), check_vma=False
    )
```

```python
import functools

import jax
import jax.numpy as jnp
from jax import lax
from jax.experimental import pallas as pl
from jax.experimental.pallas import tpu as pltpu
from jax.sharding import PartitionSpec as P

R = 256
ITERS = 5
BETA = 0.95
EPS = 1e-06
TOKENS = 65536

F32 = jnp.float32
BF16 = jnp.bfloat16
MESH = pl.DeviceIdType.MESH


def own_of(x, zl, y, c):
    return ((x * 2 + zl) * 4 + y) * 2 + c


def reduce_kernel(
    x_hbm, cot_hbm, gate_ref, down_hbm, up_hbm, mix_ref, table_ref, out_ref,
    wbuf, xv, lv, gcol, pacc, sigp, sigr, xp, acc,
    s1send, s1rel, s1recv, s2f, s2send, s2recv, zf, zsend, zrecv, zag, stage, arecv,
    ld, wsend, w1r, st1r, st2r, zp1, zp2, ddr, xr, gsend, gdr, s1relr, s1r, s2r, zr, zagr, asend, ar,
):
    r = lax.axis_index("rep")
    o = lax.axis_index("own")
    c = lax.rem(o, 2)
    y = lax.rem(o // 2, 4)
    zl = lax.rem(o // 8, 2)
    x = o // 16
    z = r * 2 + zl
    m = (x * 4 + y) * 2 + c
    sgn = 2 * zl - 1
    partner = (r, own_of(x, zl, y, 1 - c))

    xs = [lax.rem(x + d, 4) for d in range(4)]
    ys = [lax.rem(y + d, 4) for d in range(4)]
    cs = [c, 1 - c]
    x_part = [v * 16 + zl * 8 for v in xs]
    y_part = [v * 2 for v in ys]
    zs = [lax.rem(z + d, 8) for d in range(8)]

    def along(axis, d):
        if axis == 0:
            return (r, x_part[d % 4] + y_part[0] + c)
        return (r, x_part[0] + y_part[d % 4] + c)

    def zpeer(d):
        zz = zs[d % 8]
        return (lax.div(zz, 2), x * 16 + lax.rem(zz, 2) * 8 + y_part[0] + c)

    def plane(dx, dy, dc):
        return (r, x_part[dx % 4] + y_part[dy % 4] + cs[dc])

    def place(dx, dy, dc):
        return xs[dx % 4] * 8 + y_part[dy % 4] + cs[dc]

    def length(d):
        return min(d, 4 - d)

    offsets = [(dx, dy, dc) for dx in range(4) for dy in range(4) for dc in range(2)][1:]
    offsets.sort(key=lambda t: -(length(t[0]) + length(t[1])))

    quarter = [r, lax.rem(r + sgn + 4, 4), lax.rem(r - sgn + 4, 4), lax.rem(r + 2, 4)]

    pending = []

    def send(src, dst, ssem, rsem, dev):
        cp = pltpu.make_async_remote_copy(
            src_ref=src, dst_ref=dst, send_sem=ssem, recv_sem=rsem,
            device_id=dev, device_id_type=MESH,
        )
        cp.start()
        pending.append(cp)

    def arrived(dst, rsem, dev):
        pltpu.make_async_remote_copy(
            src_ref=dst, dst_ref=dst, send_sem=rsem, recv_sem=rsem,
            device_id=dev, device_id_type=MESH,
        ).wait_recv()

    loads = [
        pltpu.make_async_copy(down_hbm, wbuf.at[0, 0], ld.at[0]),
        pltpu.make_async_copy(up_hbm, wbuf.at[0, 1], ld.at[1]),
    ]
    for s in range(4):
        cols = pl.ds(pl.multiple_of(quarter[s] * 2048, 2048), 2048)
        loads.append(pltpu.make_async_copy(x_hbm.at[:, cols], xv.at[:, cols], ld.at[2 + 2 * s]))
        loads.append(pltpu.make_async_copy(cot_hbm.at[:, cols], lv.at[:, cols], ld.at[3 + 2 * s]))
    for cp in loads:
        cp.start()

    barrier = pltpu.get_barrier_semaphore()

    for d in (4, 3, 5):
        pl.semaphore_signal(barrier, inc=1, device_id=zpeer(d), device_id_type=MESH)
    for off in offsets:
        pl.semaphore_signal(barrier, inc=1, device_id=plane(*off), device_id_type=MESH)
    for d in (2, 6, 1, 7):
        pl.semaphore_signal(barrier, inc=1, device_id=zpeer(d), device_id_type=MESH)
    pl.semaphore_wait(barrier, 38)

    pos = (x, y)
    nws = [0]

    def wsem():
        nws[0] += 1
        return wsend.at[nws[0] - 1]

    def unit(s, k):
        return 16 if (s, k) in ((1, 1), (2, 0)) else 32

    def base(s, cc, k):
        return cc * 1024 + (16 * unit(s, 0) if k else 0)

    def piece(s, k, p1, p2):
        u = unit(s, k)
        return pl.ds(pl.multiple_of(base(s, c, k) + (p2 * 4 + p1) * u, u), u)

    def group(s, k, p2):
        u = 4 * unit(s, k)
        return pl.ds(pl.multiple_of(base(s, c, k) + p2 * u, u), u)

    def straight(cc, n):
        return pl.ds(pl.multiple_of(cc * 1024 + 768 + n * 64, 64), 64)

    def p12(k):
        return (pos[0], pos[1]) if k == 0 else (pos[1], pos[0])

    def near(p, d):
        return lax.rem(p + d + 4, 4)

    loads[0].wait()
    loads[1].wait()
    zdest = [
        (lax.rem(r + sgn + 4, 4), own_of(x, 1 - zl, y, c)),
        (lax.rem(r + sgn + 4, 4), own_of(x, zl, y, c)),
        (lax.rem(r + 2, 4), own_of(x, 1 - zl, y, c)),
    ]
    for s in (3, 1, 2):
        for k in range(2):
            rows = piece(s, k, *p12(k))
            send(
                wbuf.at[0, :, rows, :], wbuf.at[s, :, rows, :],
                wsem(), w1r.at[s - 1, k], zdest[s - 1],
            )
    for n in range(4):
        rows = straight(c, n)
        send(wbuf.at[0, :, rows, :], wbuf.at[1, :, rows, :], wsem(), zp1.at[n], zdest[0])
    pair = (r, own_of(x, 1 - zl, y, c))

    def pass_on(n):
        rows = straight(c, n)
        arrived(wbuf.at[1, :, rows, :], zp1.at[n], pair)
        send(wbuf.at[1, :, rows, :], wbuf.at[2, :, rows, :], wsem(), zp2.at[n], pair)

    def rows_at(s, k, stg, d):
        p1, p2 = p12(k)
        return piece(s, k, near(p1, d), p2) if stg == 1 else group(s, k, near(p2, d))

    def s1(s):
        for k in range(2):
            rows = rows_at(s, k, 1, 0)
            arrived(wbuf.at[s, :, rows, :], w1r.at[s - 1, k], zpeer(1))
            for d in (2, 1, 3):
                send(
                    wbuf.at[s, :, rows, :], wbuf.at[s, :, rows, :],
                    wsem(), st1r.at[s - 1, k, d], along(k, d),
                )

    def s2(s):
        for k in range(2):
            for d in (1, 3, 2):
                arrived(wbuf.at[s, :, rows_at(s, k, 1, -d), :], st1r.at[s - 1, k, d], along(k, -d))
        for k in range(2):
            rows = rows_at(s, k, 2, 0)
            for i, d in enumerate((1, 3)):
                send(
                    wbuf.at[s, :, rows, :], wbuf.at[s, :, rows, :],
                    wsem(), st2r.at[s - 1, k, i], along(1 - k, d),
                )

    def f2(s):
        for k in range(2):
            for i, d in enumerate((1, 3)):
                rows = rows_at(s, k, 2, -d)
                arrived(wbuf.at[s, :, rows, :], st2r.at[s - 1, k, i], along(1 - k, -d))
                send(
                    wbuf.at[s, i, rows, :], wbuf.at[s, i, rows, :],
                    wsem(), st2r.at[s - 1, k, 2 + i], along(1 - k, d),
                )

    def stage_far(s, k):
        rows = rows_at(s, k, 2, 2)
        for i, d in enumerate((1, 3)):
            arrived(wbuf.at[s, i, rows, :], st2r.at[s - 1, k, 2 + i], along(1 - k, -d))

    def to_partner(s, rows, i):
        send(wbuf.at[s, :, rows, :], wbuf.at[s, :, rows, :], wsem(), ddr.at[i], partner)

    def gathered(cc):
        return pl.ds(pl.multiple_of(cc * 1024, 256), 768)

    def d2d(s):
        for k in range(2):
            stage_far(s, k)
        to_partner(s, gathered(c), s - 1)

    def d2d_straight1():
        to_partner(1, pl.ds(pl.multiple_of(c * 1024 + 768, 256), 256), 2)

    def d2d_straight2(n):
        arrived(wbuf.at[2, :, straight(c, n), :], zp2.at[n], pair)
        to_partner(2, straight(c, n), 3 + n)

    def d2d_last(far):
        for k in range(2):
            if far:
                stage_far(3, k)
            for i, d in ((3, 2),) if far else ((0, 0), (1, -1), (2, 1)):
                to_partner(3, rows_at(3, k, 2, d), 7 + k * 4 + i)

    def from_partner(s):
        if s < 3:
            arrived(wbuf.at[s, :, gathered(1 - c), :], ddr.at[s - 1], partner)
        if s == 1:
            rows = pl.ds(pl.multiple_of((1 - c) * 1024 + 768, 256), 256)
            arrived(wbuf.at[1, :, rows, :], ddr.at[2], partner)
        if s == 2:
            for n in range(4):
                arrived(wbuf.at[2, :, straight(1 - c, n), :], ddr.at[3 + n], partner)
        if s == 3:
            for k in range(2):
                for i, d in enumerate((0, -1, 1, 2)):
                    _, p2 = p12(k)
                    rows = pl.ds(
                        pl.multiple_of(base(3, 1 - c, k) + near(p2, d) * 128, 128), 128
                    )
                    arrived(wbuf.at[3, :, rows, :], ddr.at[7 + k * 4 + i], partner)
        matmul(s, 1 - c)

    def cols_of(s):
        return pl.ds(pl.multiple_of(quarter[s] * 2048, 2048), 2048)

    def share(s):
        loads[2 + 2 * s].wait()
        send(xv.at[:, cols_of(s)], xp.at[:, cols_of(s)], wsem(), xr.at[s], partner)

    def lift(s, first, last):
        if first == 0:
            loads[3 + 2 * s].wait()

        def body(i, carry):
            cols = pl.ds(pl.multiple_of(quarter[s] * 2048 + i * 128, 128), 128)
            g = gcol[...]
            lv[:, cols] = (g * xv[:, cols].astype(F32) * lv[:, cols].astype(F32)).astype(BF16)
            return carry

        lax.fori_loop(first, last, body, 0)

    def matmul(s, cc):
        def body(i, carry):
            start = cc * 1024 + i * 512
            rows = pl.ds(pl.multiple_of(start, 512), 512)
            cols = pl.ds(pl.multiple_of(quarter[s] * 2048 + start, 512), 512)
            pacc[0] += jnp.dot(xv[:, cols], wbuf[s, 0, rows, :], preferred_element_type=F32)
            pacc[1] += jnp.dot(lv[:, cols], wbuf[s, 1, rows, :], preferred_element_type=F32)
            return carry

        lax.fori_loop(0, 2, body, 0)

    gcol[...] = jnp.transpose(jnp.broadcast_to(gate_ref[...], (128, 256)))
    pacc[...] = jnp.zeros_like(pacc)
    for s in range(4):
        share(s)
    lift(0, 0, 8)
    s1(1)
    s1(2)
    lift(0, 8, 16)
    s1(3)
    s2(1)
    pass_on(0)
    s2(2)
    pass_on(1)
    lift(1, 0, 8)
    pass_on(2)
    s2(3)
    pass_on(3)
    f2(1)
    d2d_straight1()
    lift(1, 8, 16)
    matmul(0, c)
    d2d_straight2(0)
    d2d_straight2(1)
    f2(2)
    lift(2, 0, 16)
    d2d_straight2(2)
    d2d_straight2(3)
    matmul(0, 1 - c)
    f2(3)
    d2d_last(False)
    lift(3, 0, 8)
    d2d(1)
    matmul(1, c)
    lift(3, 8, 16)
    d2d(2)
    matmul(2, c)
    from_partner(1)
    d2d_last(True)
    matmul(3, c)
    from_partner(2)
    from_partner(3)

    inner = jnp.tanh(pacc[0]).astype(BF16)
    outer = jnp.tanh(jnp.dot(inner, mix_ref[...], preferred_element_type=F32))
    slope = (pacc[1] * (1.0 - outer * outer)).astype(BF16)
    through = lax.dot_general(
        slope, mix_ref[...], (((1,), (1,)), ((), ())), preferred_element_type=F32
    )
    inner_wide = inner.astype(F32)
    signal = through * (1.0 - inner_wide * inner_wide)
    sigp[...] = jnp.transpose(signal).astype(BF16)
    other_rows = pl.ds(pl.multiple_of((1 - c) * 128, 128), 128)
    own_rows = pl.ds(pl.multiple_of(c * 128, 128), 128)

    ngs = [0]

    def gsem():
        ngs[0] += 1
        return gsend.at[ngs[0] - 1]

    send(sigp.at[other_rows], sigr, gsem(), gdr, partner)

    def own_tokens(i, carry):
        cols = pl.ds(pl.multiple_of(i * 256, 256), 256)
        acc[i] = jnp.dot(sigp[own_rows, :], xv[:, cols], preferred_element_type=F32)
        return carry

    lax.fori_loop(0, 32, own_tokens, 0, unroll=4)
    for s in range(4):
        arrived(xp.at[:, cols_of(s)], xr.at[s], partner)
    arrived(sigr, gdr, partner)

    def rows16(k, d):
        i = near(pos[k], d)
        return pl.ds(pl.multiple_of(k * 64 + i * 16, 16), 16)

    def merge(g):
        role, d = (2, -1) if g % 2 == 0 else (1, 1)

        def body(i, carry):
            b = g * 8 + i
            cols = pl.ds(pl.multiple_of(b * 256, 256), 256)
            acc[b] += jnp.dot(sigr[...], xp[:, cols], preferred_element_type=F32)
            for k in range(2):
                s1send[k, 0, b] = acc[b, rows16(k, 2), :].astype(BF16)
                s1send[k, role, b] = acc[b, rows16(k, d), :].astype(BF16)
            return carry

        lax.fori_loop(0, 8, body, 0, unroll=4)

    def far_out(g):
        side, rnd = g % 2, g // 2
        blk, rel = pl.ds(g * 8, 8), pl.ds(rnd * 8, 8)
        for k in range(2):
            send(
                s1send.at[k, 0, blk], s1rel.at[k, side, rel], gsem(),
                s1relr.at[k, side, rnd], along(k, 1 - 2 * side),
            )

    def near_out(g, role):
        blk = pl.ds(g * 8, 8)
        for k in range(2):
            send(
                s1send.at[k, role, blk], s1recv.at[k, role - 1, blk], gsem(),
                s1r.at[k, role - 1, g], along(k, 3 - 2 * role),
            )

    def relay(g):
        side, rnd = g % 2, g // 2
        rel = pl.ds(rnd * 8, 8)
        d = 1 - 2 * side
        for k in range(2):
            arrived(s1rel.at[k, side, rel], s1relr.at[k, side, rnd], along(k, -d))

            def body(i, carry, k=k):
                b = g * 8 + i
                s1send[k, 1 + side, b] = (
                    acc[b, rows16(k, d), :] + s1rel[k, side, rnd * 8 + i].astype(F32)
                ).astype(BF16)
                return carry

            lax.fori_loop(0, 8, body, 0)
        near_out(g, 1 + side)

    def finish(rnd):
        half = pl.ds(rnd * 128, 128)
        for k in range(2):
            for role in range(2):
                for g in (2 * rnd, 2 * rnd + 1):
                    arrived(
                        s1recv.at[k, role, pl.ds(g * 8, 8)], s1r.at[k, role, g],
                        along(k, 2 * role - 1),
                    )

            def own_sum(i, carry, k=k):
                tot = []
                for q in range(2):
                    b = i * 2 + q
                    tot.append(
                        acc[b, rows16(k, 0), :]
                        + s1recv[k, 0, b].astype(F32)
                        + s1recv[k, 1, b].astype(F32)
                    )
                rows = pl.ds(pl.multiple_of(i * 16, 16), 16)
                for j in range(4):
                    a, h = j // 2, j % 2
                    part = jnp.concatenate(
                        [t[a * 8 : a * 8 + 8, h * 128 : h * 128 + 128] for t in tot], axis=0
                    )
                    s2f[k, j, rows, :] = part
                    s2send[k, j, rows, :] = part.astype(BF16)
                return carry

            lax.fori_loop(rnd * 8, rnd * 8 + 8, own_sum, 0)
            for d in (2, 1, 3):
                j = near(pos[1 - k], d)
                send(
                    s2send.at[k, j, half], s2recv.at[k, d - 1, half], gsem(),
                    s2r.at[k, d - 1, rnd], along(1 - k, d),
                )

    merge(0)
    far_out(0)
    near_out(0, 2)
    merge(1)
    far_out(1)
    near_out(1, 1)
    merge(2)
    far_out(2)
    merge(3)
    far_out(3)
    relay(0)
    near_out(3, 1)
    relay(1)
    near_out(2, 2)
    relay(2)
    finish(0)
    relay(3)
    finish(1)

    parts = []
    for k in range(2):
        tot = s2f[k, pos[1 - k]]
        for d in (1, 3, 2):
            for rnd in range(2):
                half = pl.ds(rnd * 128, 128)
                arrived(s2recv.at[k, d - 1, half], s2r.at[k, d - 1, rnd], along(1 - k, -d))
            tot = tot + s2recv[k, d - 1].astype(F32)
        parts.append(tot.reshape(32, 8, 128))
    both = jnp.concatenate(parts, axis=1)
    zf[...] = both
    zsend[...] = both.astype(BF16)

    for d in (4, 3, 5, 2, 6, 1, 7):
        zz = lax.rem(z + d, 8)
        send(zsend.at[pl.ds(zz * 4, 4)], zrecv.at[d - 1], gsem(), zr.at[d - 1], zpeer(d))
    tot = zf[pl.ds(z * 4, 4)]
    for d in (1, 7, 2, 6, 3, 5, 4):
        arrived(zrecv.at[d - 1], zr.at[d - 1], zpeer(-d))
        tot = tot + zrecv[d - 1].astype(F32)
    mine = pl.ds(z * 4, 4)
    zag[mine] = tot.astype(BF16)
    for d in (4, 3, 5, 2, 6, 1, 7):
        send(zag.at[mine], zag.at[mine], gsem(), zagr.at[d - 1], zpeer(d))
    for d in (1, 7, 2, 6, 3, 5, 4):
        zz = lax.rem(z - d + 8, 8)
        arrived(zag.at[pl.ds(zz * 4, 4)], zagr.at[d - 1], zpeer(-d))

    for e, off in enumerate(offsets):
        stage[e] = zag[jnp.maximum(table_ref[plane(*off)[1]], 0)]
    arecv[m] = zag[jnp.maximum(table_ref[o], 0)]
    for e, off in enumerate(offsets):
        pltpu.make_async_remote_copy(
            src_ref=stage.at[e], dst_ref=arecv.at[m], send_sem=asend, recv_sem=ar.at[e],
            device_id=plane(*off), device_id_type=MESH,
        ).start()
    for cp in pending:
        cp.wait_send()
    for e, (dx, dy, dc) in reversed(list(enumerate(offsets))):
        arrived(arecv.at[place(-dx, -dy, dc)], ar.at[e], plane(-dx, -dy, dc))
    for xx in range(4):
        for yy in range(4):
            for cc in range(2):
                tile = arecv[(xx * 4 + yy) * 2 + cc]
                r0 = cc * 128 + xx * 16 + (yy // 2) * 8
                l0 = (yy % 2) * 128
                out_ref[r0 : r0 + 8, l0 : l0 + 128] = tile[0:8]
                r1 = cc * 128 + 64 + yy * 16 + (xx // 2) * 8
                l1 = (xx % 2) * 128
                out_ref[r1 : r1 + 8, l1 : l1 + 128] = tile[8:16]

    first = pl.ds(0, 31)
    pltpu.make_async_remote_copy(
        src_ref=stage.at[first], dst_ref=arecv.at[first], send_sem=asend, recv_sem=asend,
        device_id=partner, device_id_type=MESH,
    ).wait_send()


def reduced_block(inputs, cotangent, gate, down_weight, up_weight, mixing, table):
    any_spec = pl.BlockSpec(memory_space=pltpu.HBM)
    vm = pl.BlockSpec(memory_space=pltpu.VMEM)
    dma = pltpu.SemaphoreType.DMA
    V = pltpu.VMEM
    return pl.pallas_call(
        reduce_kernel,
        name="reduce",
        out_shape=jax.ShapeDtypeStruct((256, 256), BF16),
        in_specs=[any_spec, any_spec, vm, any_spec, any_spec, vm,
                  pl.BlockSpec(memory_space=pltpu.SMEM)],
        out_specs=vm,
        scratch_shapes=[
            V((4, 2, 2048, 256), BF16),
            V((256, 8192), BF16),
            V((256, 8192), BF16),
            V((256, 128), F32),
            V((2, 256, 256), F32),
            V((256, 256), BF16),
            V((128, 256), BF16),
            V((256, 8192), BF16),
            V((32, 128, 256), F32),
            V((2, 3, 32, 16, 256), BF16),
            V((2, 2, 16, 16, 256), BF16),
            V((2, 2, 32, 16, 256), BF16),
            V((2, 4, 256, 128), F32),
            V((2, 4, 256, 128), BF16),
            V((2, 3, 256, 128), BF16),
            V((32, 16, 128), F32),
            V((32, 16, 128), BF16),
            V((7, 4, 16, 128), BF16),
            V((32, 16, 128), BF16),
            V((32, 16, 128), BF16),
            V((32, 16, 128), BF16),
            dma((10,)),
            dma((94,)),
            dma((3, 2)),
            dma((3, 2, 4)),
            dma((3, 2, 4)),
            dma((4,)),
            dma((4,)),
            dma((15,)),
            dma((4,)),
            dma((54,)),
            dma,
            dma((2, 2, 2)),
            dma((2, 2, 4)),
            dma((2, 3, 2)),
            dma((7,)),
            dma((7,)),
            dma,
            dma((31,)),
        ],
        compiler_params=pltpu.CompilerParams(
            collective_id=0, has_side_effects=True, vmem_limit_bytes=63 * 1024 * 1024
        ),
    )(inputs, cotangent, gate, down_weight, up_weight, mixing, table)


def halves(a):
    hi = a.astype(BF16)
    return hi, (a - hi.astype(F32)).astype(BF16)


def dot(a, b):
    return jnp.dot(a, b, preferred_element_type=F32)


def product(a, b):
    (ah, al), (bh, bl) = a, b
    lhs = jnp.concatenate([ah, ah, al], axis=1)
    rhs = jnp.concatenate([bh, bl, bh], axis=0)
    return dot(lhs, rhs)


def root_kernel(gt_ref, left_ref, right_ref, table_ref, out_ref, norms, results):
    eye = (
        lax.broadcasted_iota(jnp.int32, (R, R), 0) == lax.broadcasted_iota(jnp.int32, (R, R), 1)
    ).astype(F32)
    scaled = gt_ref[...].astype(F32) * (1.0 / TOKENS)
    gt = scaled.astype(BF16)
    g = jnp.transpose(scaled).astype(BF16)
    news = [
        BETA * left_ref[0] + (1.0 - BETA) * dot(g, gt),
        BETA * right_ref[0] + (1.0 - BETA) * dot(gt, g),
    ]
    for i, a in enumerate(news):
        shifted = a + EPS * eye
        norm = jnp.sqrt(jnp.sum(shifted * shifted, keepdims=True))
        m = shifted / norm
        results[i] = lax.rsqrt(jnp.sqrt(norm)) * ((5.0 * eye - m) / 4.0)
        norms[i] = m

    def advance(m, mb):
        e = dot(mb, mb) * (1.0 / 16.0) - m * (10.0 / 16.0)
        eb = e.astype(BF16)
        h = (25.0 / 8.0) * e + dot(eb, eb)
        return (625.0 / 256.0) * m + dot(h.astype(BF16), mb)

    def multiply(x, mb):
        return 1.25 * x - 0.25 * dot(x.astype(BF16), mb)

    for i in range(2):
        norms[i] = advance(norms[i], norms[i].astype(BF16))

    def sweep(step, carry):
        for i in range(2):
            m = norms[i]
            mb = m.astype(BF16)
            results[i] = multiply(results[i], mb)
            norms[i] = advance(m, mb)
        return carry

    lax.fori_loop(0, ITERS - 2, sweep, 0)
    left, right = [multiply(results[i], norms[i].astype(BF16)) for i in range(2)]
    half = dot(jnp.concatenate(halves(left), axis=1), jnp.concatenate([g, g], axis=0))
    done = product(halves(half), halves(right))
    filled = table_ref[lax.axis_index("own")] >= 0
    out_ref[...] = jnp.where(filled, done, 0.0)


def preconditioned(gt, left, right, table):
    vm = pl.BlockSpec(memory_space=pltpu.VMEM)
    return pl.pallas_call(
        root_kernel,
        name="roots",
        out_shape=jax.ShapeDtypeStruct((R, R), F32),
        in_specs=[vm, vm, vm, pl.BlockSpec(memory_space=pltpu.SMEM)],
        out_specs=vm,
        scratch_shapes=[pltpu.VMEM((2, R, R), F32), pltpu.VMEM((2, R, R), F32)],
        compiler_params=pltpu.CompilerParams(vmem_limit_bytes=16 * 1024 * 1024),
    )(gt, left, right, table)


def shards(
    inputs, cotangent, gate, down_weight, up_weight, mixing, owner_table, left_factor, right_factor
):
    table = owner_table.reshape(-1)
    gt = reduced_block(
        inputs, cotangent, gate.reshape(1, -1), down_weight, up_weight, mixing, table
    )
    return preconditioned(gt, left_factor, right_factor, table)


def solution(mesh):
    in_specs = (
        P(("rep", "own"), None),
        P(("rep", "own"), None),
        P(("rep", "own")),
        P("rep", None),
        P("rep", None),
        P(),
        P(),
        P("own", None, None),
        P("own", None, None),
    )
    return jax.shard_map(
        shards, mesh=mesh, in_specs=in_specs, out_specs=P("own", None), check_vma=False
    )
```

```python
import functools

import jax
import jax.numpy as jnp
from jax import lax
from jax.experimental import pallas as pl
from jax.experimental.pallas import tpu as pltpu
from jax.sharding import PartitionSpec as P

R = 256
ITERS = 5
BETA = 0.95
EPS = 1e-06
TOKENS = 65536

F32 = jnp.float32
BF16 = jnp.bfloat16
MESH = pl.DeviceIdType.MESH


def own_of(x, zl, y, c):
    return ((x * 2 + zl) * 4 + y) * 2 + c


def reduce_kernel(
    x_hbm, cot_hbm, gate_hbm, down_hbm, up_hbm, mix_hbm, table_hbm, left_hbm, right_hbm, out_ref,
    wbuf, xv, lv, gcol, pacc, sigp, sigr, xp, acc,
    s1send, s1rel, s1recv, s2f, s2send, s2recv, zf, zsend, zrecv, zag, stage, arecv, factors, gtv, norms, results, gate_ref, mix_ref, table_ref,
    ld, wsend, w1r, st1r, st2r, zp1, zp2, ddr, xr, gsend, gdr, s1relr, s1r, s2r, zr, zagr, asend, ar,
):
    r = lax.axis_index("rep")
    o = lax.axis_index("own")
    c = lax.rem(o, 2)
    y = lax.rem(o // 2, 4)
    zl = lax.rem(o // 8, 2)
    x = o // 16
    z = r * 2 + zl
    m = (x * 4 + y) * 2 + c
    sgn = 2 * zl - 1
    partner = (r, own_of(x, zl, y, 1 - c))

    xs = [lax.rem(x + d, 4) for d in range(4)]
    ys = [lax.rem(y + d, 4) for d in range(4)]
    cs = [c, 1 - c]
    x_part = [v * 16 + zl * 8 for v in xs]
    y_part = [v * 2 for v in ys]
    zs = [lax.rem(z + d, 8) for d in range(8)]

    def along(axis, d):
        if axis == 0:
            return (r, x_part[d % 4] + y_part[0] + c)
        return (r, x_part[0] + y_part[d % 4] + c)

    def zpeer(d):
        zz = zs[d % 8]
        return (lax.div(zz, 2), x * 16 + lax.rem(zz, 2) * 8 + y_part[0] + c)

    def plane(dx, dy, dc):
        return (r, x_part[dx % 4] + y_part[dy % 4] + cs[dc])

    def place(dx, dy, dc):
        return xs[dx % 4] * 8 + y_part[dy % 4] + cs[dc]

    def length(d):
        return min(d, 4 - d)

    offsets = [(dx, dy, dc) for dx in range(4) for dy in range(4) for dc in range(2)][1:]
    offsets.sort(key=lambda t: -(length(t[0]) + length(t[1])))

    quarter = [r, lax.rem(r + sgn + 4, 4), lax.rem(r - sgn + 4, 4), lax.rem(r + 2, 4)]

    pending = []

    def send(src, dst, ssem, rsem, dev):
        cp = pltpu.make_async_remote_copy(
            src_ref=src, dst_ref=dst, send_sem=ssem, recv_sem=rsem,
            device_id=dev, device_id_type=MESH,
        )
        cp.start()
        pending.append(cp)

    def arrived(dst, rsem, dev):
        pltpu.make_async_remote_copy(
            src_ref=dst, dst_ref=dst, send_sem=rsem, recv_sem=rsem,
            device_id=dev, device_id_type=MESH,
        ).wait_recv()

    loads = [
        pltpu.make_async_copy(down_hbm, wbuf.at[0, 0], ld.at[0]),
        pltpu.make_async_copy(up_hbm, wbuf.at[0, 1], ld.at[1]),
    ]
    for s in range(4):
        cols = pl.ds(pl.multiple_of(quarter[s] * 2048, 2048), 2048)
        loads.append(pltpu.make_async_copy(x_hbm.at[:, cols], xv.at[:, cols], ld.at[2 + 2 * s]))
        loads.append(pltpu.make_async_copy(cot_hbm.at[:, cols], lv.at[:, cols], ld.at[3 + 2 * s]))
    loads.append(pltpu.make_async_copy(left_hbm, factors.at[pl.ds(0, 1)], ld.at[10]))
    loads.append(pltpu.make_async_copy(right_hbm, factors.at[pl.ds(1, 1)], ld.at[11]))
    loads.append(pltpu.make_async_copy(gate_hbm, gate_ref, ld.at[12]))
    loads.append(pltpu.make_async_copy(mix_hbm, mix_ref, ld.at[13]))
    loads.append(pltpu.make_async_copy(table_hbm, table_ref, ld.at[14]))
    for cp in loads:
        cp.start()

    barrier = pltpu.get_barrier_semaphore()

    for d in (4, 3, 5):
        pl.semaphore_signal(barrier, inc=1, device_id=zpeer(d), device_id_type=MESH)
    for off in offsets:
        pl.semaphore_signal(barrier, inc=1, device_id=plane(*off), device_id_type=MESH)
    for d in (2, 6, 1, 7):
        pl.semaphore_signal(barrier, inc=1, device_id=zpeer(d), device_id_type=MESH)
    pl.semaphore_wait(barrier, 38)

    pos = (x, y)
    nws = [0]

    def wsem():
        nws[0] += 1
        return wsend.at[nws[0] - 1]

    def unit(s, k):
        return 32 if s == 3 else 16

    def base(s, cc, k):
        return cc * 1024 + (16 * unit(s, 0) if k else 0)

    def piece(s, k, p1, p2):
        u = unit(s, k)
        return pl.ds(pl.multiple_of(base(s, c, k) + (p2 * 4 + p1) * u, u), u)

    def group(s, k, p2):
        u = 4 * unit(s, k)
        return pl.ds(pl.multiple_of(base(s, c, k) + p2 * u, u), u)

    def straight(cc, n):
        size = 128 if n < 3 else 64
        start = 512 + 128 * min(n, 3) + 64 * max(n - 3, 0)
        return pl.ds(pl.multiple_of(cc * 1024 + start, 64), size)

    def p12(k):
        return (pos[0], pos[1]) if k == 0 else (pos[1], pos[0])

    def near(p, d):
        return lax.rem(p + d + 4, 4)

    loads[0].wait()
    loads[1].wait()
    zdest = [
        (lax.rem(r + sgn + 4, 4), own_of(x, 1 - zl, y, c)),
        (lax.rem(r + sgn + 4, 4), own_of(x, zl, y, c)),
        (lax.rem(r + 2, 4), own_of(x, 1 - zl, y, c)),
    ]
    for s in (3, 1, 2):
        for k in range(2):
            rows = piece(s, k, *p12(k))
            send(
                wbuf.at[0, :, rows, :], wbuf.at[s, :, rows, :],
                wsem(), w1r.at[s - 1, k], zdest[s - 1],
            )
    for n in range(5):
        rows = straight(c, n)
        send(wbuf.at[0, :, rows, :], wbuf.at[1, :, rows, :], wsem(), zp1.at[n], zdest[0])
    pair = (r, own_of(x, 1 - zl, y, c))

    def pass_on(n):
        rows = straight(c, n)
        arrived(wbuf.at[1, :, rows, :], zp1.at[n], pair)
        send(wbuf.at[1, :, rows, :], wbuf.at[2, :, rows, :], wsem(), zp2.at[n], pair)

    def rows_at(s, k, stg, d):
        p1, p2 = p12(k)
        return piece(s, k, near(p1, d), p2) if stg == 1 else group(s, k, near(p2, d))

    def s1(s):
        for k in range(2):
            rows = rows_at(s, k, 1, 0)
            arrived(wbuf.at[s, :, rows, :], w1r.at[s - 1, k], zpeer(1))
            for d in (2, 1, 3):
                send(
                    wbuf.at[s, :, rows, :], wbuf.at[s, :, rows, :],
                    wsem(), st1r.at[s - 1, k, d], along(k, d),
                )

    def s2(s):
        for k in range(2):
            for d in (1, 3, 2):
                arrived(wbuf.at[s, :, rows_at(s, k, 1, -d), :], st1r.at[s - 1, k, d], along(k, -d))
        for k in range(2):
            rows = rows_at(s, k, 2, 0)
            for i, d in enumerate((1, 3)):
                send(
                    wbuf.at[s, :, rows, :], wbuf.at[s, :, rows, :],
                    wsem(), st2r.at[s - 1, k, i], along(1 - k, d),
                )

    def f2(s):
        for k in range(2):
            for i, d in enumerate((1, 3)):
                rows = rows_at(s, k, 2, -d)
                arrived(wbuf.at[s, :, rows, :], st2r.at[s - 1, k, i], along(1 - k, -d))
                send(
                    wbuf.at[s, i, rows, :], wbuf.at[s, i, rows, :],
                    wsem(), st2r.at[s - 1, k, 2 + i], along(1 - k, d),
                )

    def stage_far(s, k):
        rows = rows_at(s, k, 2, 2)
        for i, d in enumerate((1, 3)):
            arrived(wbuf.at[s, i, rows, :], st2r.at[s - 1, k, 2 + i], along(1 - k, -d))

    def to_partner(s, rows, i):
        send(wbuf.at[s, :, rows, :], wbuf.at[s, :, rows, :], wsem(), ddr.at[i], partner)

    def gathered(cc):
        return pl.ds(pl.multiple_of(cc * 1024, 512), 512)

    def d2d(s):
        for k in range(2):
            stage_far(s, k)
        to_partner(s, gathered(c), s - 1)

    def d2d_straight1():
        to_partner(1, pl.ds(pl.multiple_of(c * 1024 + 512, 512), 512), 2)

    def d2d_straight2(n):
        arrived(wbuf.at[2, :, straight(c, n), :], zp2.at[n], pair)
        to_partner(2, straight(c, n), 3 + n)

    def d2d_last(far):
        for k in range(2):
            if far:
                stage_far(3, k)
            for i, d in ((3, 2),) if far else ((0, 0), (1, -1), (2, 1)):
                to_partner(3, rows_at(3, k, 2, d), 8 + k * 4 + i)

    def from_partner(s):
        if s < 3:
            arrived(wbuf.at[s, :, gathered(1 - c), :], ddr.at[s - 1], partner)
        if s == 1:
            rows = pl.ds(pl.multiple_of((1 - c) * 1024 + 512, 512), 512)
            arrived(wbuf.at[1, :, rows, :], ddr.at[2], partner)
        if s == 2:
            for n in range(5):
                arrived(wbuf.at[2, :, straight(1 - c, n), :], ddr.at[3 + n], partner)
        if s == 3:
            for k in range(2):
                for i, d in enumerate((0, -1, 1, 2)):
                    _, p2 = p12(k)
                    rows = pl.ds(
                        pl.multiple_of(base(3, 1 - c, k) + near(p2, d) * 128, 128), 128
                    )
                    arrived(wbuf.at[3, :, rows, :], ddr.at[8 + k * 4 + i], partner)
        matmul(s, 1 - c)

    def cols_of(s):
        return pl.ds(pl.multiple_of(quarter[s] * 2048, 2048), 2048)

    def share(s):
        loads[2 + 2 * s].wait()
        send(xv.at[:, cols_of(s)], xp.at[:, cols_of(s)], wsem(), xr.at[s], partner)

    def lift(s, first, last):
        if first == 0:
            loads[3 + 2 * s].wait()

        def body(i, carry):
            cols = pl.ds(pl.multiple_of(quarter[s] * 2048 + i * 128, 128), 128)
            g = gcol[...]
            lv[:, cols] = (g * xv[:, cols].astype(F32) * lv[:, cols].astype(F32)).astype(BF16)
            return carry

        lax.fori_loop(first, last, body, 0)

    def matmul(s, cc):
        def body(i, carry):
            start = cc * 1024 + i * 512
            rows = pl.ds(pl.multiple_of(start, 512), 512)
            cols = pl.ds(pl.multiple_of(quarter[s] * 2048 + start, 512), 512)
            pacc[0] += jnp.dot(xv[:, cols], wbuf[s, 0, rows, :], preferred_element_type=F32)
            pacc[1] += jnp.dot(lv[:, cols], wbuf[s, 1, rows, :], preferred_element_type=F32)
            return carry

        lax.fori_loop(0, 2, body, 0)

    loads[12].wait()
    gcol[...] = jnp.transpose(jnp.broadcast_to(gate_ref[...], (128, 256)))
    pacc[...] = jnp.zeros_like(pacc)
    for s in range(4):
        share(s)
    lift(0, 0, 8)
    s1(1)
    s1(2)
    lift(0, 8, 16)
    s1(3)
    s2(1)
    s2(2)
    pass_on(0)
    lift(1, 0, 8)
    s2(3)
    pass_on(1)
    f2(1)
    lift(1, 8, 16)
    pass_on(2)
    f2(2)
    matmul(0, c)
    pass_on(3)
    lift(2, 0, 8)
    f2(3)
    d2d_last(False)
    d2d_straight2(0)
    pass_on(4)
    d2d_straight1()
    d2d(1)
    lift(2, 8, 16)
    d2d_straight2(1)
    d2d(2)
    lift(3, 0, 16)
    matmul(0, 1 - c)
    matmul(1, c)
    d2d_straight2(2)
    d2d_last(True)
    matmul(3, c)
    from_partner(1)
    d2d_straight2(3)
    from_partner(3)
    d2d_straight2(4)
    matmul(2, c)
    from_partner(2)

    loads[13].wait()
    loads[14].wait()
    inner = jnp.tanh(pacc[0]).astype(BF16)
    outer = jnp.tanh(jnp.dot(inner, mix_ref[...], preferred_element_type=F32))
    slope = (pacc[1] * (1.0 - outer * outer)).astype(BF16)
    through = lax.dot_general(
        slope, mix_ref[...], (((1,), (1,)), ((), ())), preferred_element_type=F32
    )
    inner_wide = inner.astype(F32)
    signal = through * (1.0 - inner_wide * inner_wide)
    sigp[...] = jnp.transpose(signal).astype(BF16)
    other_rows = pl.ds(pl.multiple_of((1 - c) * 128, 128), 128)
    own_rows = pl.ds(pl.multiple_of(c * 128, 128), 128)

    ngs = [0]

    def gsem():
        ngs[0] += 1
        return gsend.at[ngs[0] - 1]

    send(sigp.at[other_rows], sigr, gsem(), gdr, partner)

    def own_tokens(i, carry):
        cols = pl.ds(pl.multiple_of(i * 256, 256), 256)
        acc[i] = jnp.dot(sigp[own_rows, :], xv[:, cols], preferred_element_type=F32)
        return carry

    lax.fori_loop(0, 32, own_tokens, 0, unroll=4)
    for s in range(4):
        arrived(xp.at[:, cols_of(s)], xr.at[s], partner)
    arrived(sigr, gdr, partner)

    def rows16(k, d):
        i = near(pos[k], d)
        return pl.ds(pl.multiple_of(k * 64 + i * 16, 16), 16)

    def merge(g):
        role, d = (2, -1) if g % 2 == 0 else (1, 1)

        def body(i, carry):
            b = g * 8 + i
            cols = pl.ds(pl.multiple_of(b * 256, 256), 256)
            acc[b] += jnp.dot(sigr[...], xp[:, cols], preferred_element_type=F32)
            for k in range(2):
                s1send[k, 0, b] = acc[b, rows16(k, 2), :].astype(BF16)
                s1send[k, role, b] = acc[b, rows16(k, d), :].astype(BF16)
            return carry

        lax.fori_loop(0, 8, body, 0, unroll=4)

    def far_out(g):
        side, rnd = g % 2, g // 2
        blk, rel = pl.ds(g * 8, 8), pl.ds(rnd * 8, 8)
        for k in range(2):
            send(
                s1send.at[k, 0, blk], s1rel.at[k, side, rel], gsem(),
                s1relr.at[k, side, rnd], along(k, 1 - 2 * side),
            )

    def near_out(g, role):
        blk = pl.ds(g * 8, 8)
        for k in range(2):
            send(
                s1send.at[k, role, blk], s1recv.at[k, role - 1, blk], gsem(),
                s1r.at[k, role - 1, g], along(k, 3 - 2 * role),
            )

    def relay(g):
        side, rnd = g % 2, g // 2
        rel = pl.ds(rnd * 8, 8)
        d = 1 - 2 * side
        for k in range(2):
            arrived(s1rel.at[k, side, rel], s1relr.at[k, side, rnd], along(k, -d))

            def body(i, carry, k=k):
                b = g * 8 + i
                s1send[k, 1 + side, b] = (
                    acc[b, rows16(k, d), :] + s1rel[k, side, rnd * 8 + i].astype(F32)
                ).astype(BF16)
                return carry

            lax.fori_loop(0, 8, body, 0)
        near_out(g, 1 + side)

    def finish(rnd):
        half = pl.ds(rnd * 128, 128)
        for k in range(2):
            for role in range(2):
                for g in (2 * rnd, 2 * rnd + 1):
                    arrived(
                        s1recv.at[k, role, pl.ds(g * 8, 8)], s1r.at[k, role, g],
                        along(k, 2 * role - 1),
                    )

            def own_sum(i, carry, k=k):
                tot = []
                for q in range(2):
                    b = i * 2 + q
                    tot.append(
                        acc[b, rows16(k, 0), :]
                        + s1recv[k, 0, b].astype(F32)
                        + s1recv[k, 1, b].astype(F32)
                    )
                rows = pl.ds(pl.multiple_of(i * 16, 16), 16)
                for j in range(4):
                    a, h = j // 2, j % 2
                    part = jnp.concatenate(
                        [t[a * 8 : a * 8 + 8, h * 128 : h * 128 + 128] for t in tot], axis=0
                    )
                    s2f[k, j, rows, :] = part
                    s2send[k, j, rows, :] = part.astype(BF16)
                return carry

            lax.fori_loop(rnd * 8, rnd * 8 + 8, own_sum, 0)
            for d in (2, 1, 3):
                j = near(pos[1 - k], d)
                send(
                    s2send.at[k, j, half], s2recv.at[k, d - 1, half], gsem(),
                    s2r.at[k, d - 1, rnd], along(1 - k, d),
                )

    merge(0)
    far_out(0)
    near_out(0, 2)
    merge(1)
    far_out(1)
    near_out(1, 1)
    merge(2)
    far_out(2)
    merge(3)
    far_out(3)
    relay(0)
    near_out(3, 1)
    relay(1)
    near_out(2, 2)
    relay(2)
    finish(0)
    relay(3)
    finish(1)

    parts = []
    for k in range(2):
        tot = s2f[k, pos[1 - k]]
        for d in (1, 3, 2):
            for rnd in range(2):
                half = pl.ds(rnd * 128, 128)
                arrived(s2recv.at[k, d - 1, half], s2r.at[k, d - 1, rnd], along(1 - k, -d))
            tot = tot + s2recv[k, d - 1].astype(F32)
        parts.append(tot.reshape(32, 8, 128))
    both = jnp.concatenate(parts, axis=1)
    zf[...] = both
    zsend[...] = both.astype(BF16)

    for d in (4, 3, 5, 2, 6, 1, 7):
        zz = lax.rem(z + d, 8)
        send(zsend.at[pl.ds(zz * 4, 4)], zrecv.at[d - 1], gsem(), zr.at[d - 1], zpeer(d))
    tot = zf[pl.ds(z * 4, 4)]
    for d in (1, 7, 2, 6, 3, 5, 4):
        arrived(zrecv.at[d - 1], zr.at[d - 1], zpeer(-d))
        tot = tot + zrecv[d - 1].astype(F32)
    mine = pl.ds(z * 4, 4)
    zag[mine] = tot.astype(BF16)
    for d in (4, 3, 5, 2, 6, 1, 7):
        send(zag.at[mine], zag.at[mine], gsem(), zagr.at[d - 1], zpeer(d))
    for d in (1, 7, 2, 6, 3, 5, 4):
        zz = lax.rem(z - d + 8, 8)
        arrived(zag.at[pl.ds(zz * 4, 4)], zagr.at[d - 1], zpeer(-d))

    for e, off in enumerate(offsets):
        stage[e] = zag[jnp.maximum(table_ref[plane(*off)[1]], 0)]
    arecv[m] = zag[jnp.maximum(table_ref[o], 0)]
    for e, off in enumerate(offsets):
        pltpu.make_async_remote_copy(
            src_ref=stage.at[e], dst_ref=arecv.at[m], send_sem=asend, recv_sem=ar.at[e],
            device_id=plane(*off), device_id_type=MESH,
        ).start()
    for cp in pending:
        cp.wait_send()
    for e, (dx, dy, dc) in reversed(list(enumerate(offsets))):
        arrived(arecv.at[place(-dx, -dy, dc)], ar.at[e], plane(-dx, -dy, dc))
    for xx in range(4):
        for yy in range(4):
            for cc in range(2):
                tile = arecv[(xx * 4 + yy) * 2 + cc]
                r0 = cc * 128 + xx * 16 + (yy // 2) * 8
                l0 = (yy % 2) * 128
                gtv[r0 : r0 + 8, l0 : l0 + 128] = tile[0:8].astype(F32)
                r1 = cc * 128 + 64 + yy * 16 + (xx // 2) * 8
                l1 = (xx % 2) * 128
                gtv[r1 : r1 + 8, l1 : l1 + 128] = tile[8:16].astype(F32)

    first = pl.ds(0, 31)
    pltpu.make_async_remote_copy(
        src_ref=stage.at[first], dst_ref=arecv.at[first], send_sem=asend, recv_sem=asend,
        device_id=partner, device_id_type=MESH,
    ).wait_send()
    loads[10].wait()
    loads[11].wait()
    roots(gtv, factors, norms, results, table_ref[o] >= 0, out_ref)


def reduced_block(inputs, cotangent, gate, down_weight, up_weight, mixing, table, left, right):
    any_spec = pl.BlockSpec(memory_space=pltpu.HBM)
    vm = pl.BlockSpec(memory_space=pltpu.VMEM)
    dma = pltpu.SemaphoreType.DMA
    V = pltpu.VMEM
    return pl.pallas_call(
        reduce_kernel,
        name="reduce",
        out_shape=jax.ShapeDtypeStruct((256, 256), F32),
        in_specs=[any_spec] * 9,
        out_specs=vm,
        scratch_shapes=[
            V((4, 2, 2048, 256), BF16),
            V((256, 8192), BF16),
            V((256, 8192), BF16),
            V((256, 128), F32),
            V((2, 256, 256), F32),
            V((256, 256), BF16),
            V((128, 256), BF16),
            V((256, 8192), BF16),
            V((32, 128, 256), F32),
            V((2, 3, 32, 16, 256), BF16),
            V((2, 2, 16, 16, 256), BF16),
            V((2, 2, 32, 16, 256), BF16),
            V((2, 4, 256, 128), F32),
            V((2, 4, 256, 128), BF16),
            V((2, 3, 256, 128), BF16),
            V((32, 16, 128), F32),
            V((32, 16, 128), BF16),
            V((7, 4, 16, 128), BF16),
            V((32, 16, 128), BF16),
            V((32, 16, 128), BF16),
            V((32, 16, 128), BF16),
            V((2, R, R), F32),
            V((R, R), F32),
            V((2, R, R), F32),
            V((2, R, R), F32),
            V((1, 256), F32),
            V((R, R), BF16),
            pltpu.SMEM((64,), jnp.int32),
            dma((15,)),
            dma((97,)),
            dma((3, 2)),
            dma((3, 2, 4)),
            dma((3, 2, 4)),
            dma((5,)),
            dma((5,)),
            dma((16,)),
            dma((4,)),
            dma((54,)),
            dma,
            dma((2, 2, 2)),
            dma((2, 2, 4)),
            dma((2, 3, 2)),
            dma((7,)),
            dma((7,)),
            dma,
            dma((31,)),
        ],
        compiler_params=pltpu.CompilerParams(
            collective_id=0, has_side_effects=True, vmem_limit_bytes=63 * 1024 * 1024
        ),
    )(inputs, cotangent, gate, down_weight, up_weight, mixing, table, left, right)


def halves(a):
    hi = a.astype(BF16)
    return hi, (a - hi.astype(F32)).astype(BF16)


def dot(a, b):
    return jnp.dot(a, b, preferred_element_type=F32)


def product(a, b):
    (ah, al), (bh, bl) = a, b
    lhs = jnp.concatenate([ah, ah, al], axis=1)
    rhs = jnp.concatenate([bh, bl, bh], axis=0)
    return dot(lhs, rhs)


def roots(gt_ref, factors, norms, results, filled, out_ref):
    eye = (
        lax.broadcasted_iota(jnp.int32, (R, R), 0) == lax.broadcasted_iota(jnp.int32, (R, R), 1)
    ).astype(F32)
    scaled = gt_ref[...] * (1.0 / TOKENS)
    gt = scaled.astype(BF16)
    g = jnp.transpose(scaled).astype(BF16)
    news = [
        BETA * factors[0] + (1.0 - BETA) * dot(g, gt),
        BETA * factors[1] + (1.0 - BETA) * dot(gt, g),
    ]
    for i, a in enumerate(news):
        shifted = a + EPS * eye
        norm = jnp.sqrt(jnp.sum(shifted * shifted, keepdims=True))
        m = shifted / norm
        results[i] = lax.rsqrt(jnp.sqrt(norm)) * ((5.0 * eye - m) / 4.0)
        norms[i] = m

    def advance(m, mb):
        e = dot(mb, mb) * (1.0 / 16.0) - m * (10.0 / 16.0)
        eb = e.astype(BF16)
        h = (25.0 / 8.0) * e + dot(eb, eb)
        return (625.0 / 256.0) * m + dot(h.astype(BF16), mb)

    def multiply(x, mb):
        return 1.25 * x - 0.25 * dot(x.astype(BF16), mb)

    for i in range(2):
        norms[i] = advance(norms[i], norms[i].astype(BF16))

    def sweep(step, carry):
        for i in range(2):
            m = norms[i]
            mb = m.astype(BF16)
            results[i] = multiply(results[i], mb)
            norms[i] = advance(m, mb)
        return carry

    lax.fori_loop(0, ITERS - 2, sweep, 0)
    left, right = [multiply(results[i], norms[i].astype(BF16)) for i in range(2)]
    half = dot(jnp.concatenate(halves(left), axis=1), jnp.concatenate([g, g], axis=0))
    done = product(halves(half), halves(right))
    out_ref[...] = jnp.where(filled, done, 0.0)


def shards(
    inputs, cotangent, gate, down_weight, up_weight, mixing, owner_table, left_factor, right_factor
):
    table = owner_table.reshape(-1)
    return reduced_block(
        inputs, cotangent, gate.reshape(1, -1), down_weight, up_weight, mixing, table,
        left_factor, right_factor,
    )


def solution(mesh):
    in_specs = (
        P(("rep", "own"), None),
        P(("rep", "own"), None),
        P(("rep", "own")),
        P("rep", None),
        P("rep", None),
        P(),
        P(),
        P("own", None, None),
        P("own", None, None),
    )
    return jax.shard_map(
        shards, mesh=mesh, in_specs=in_specs, out_specs=P("own", None), check_vma=False
    )
```

```python
import functools

import jax
import jax.numpy as jnp
from jax import lax
from jax.experimental import pallas as pl
from jax.experimental.pallas import tpu as pltpu
from jax.sharding import PartitionSpec as P

R = 256
ITERS = 5
BETA = 0.95
EPS = 1e-06
TOKENS = 65536

F32 = jnp.float32
BF16 = jnp.bfloat16
MESH = pl.DeviceIdType.MESH


def own_of(x, zl, y, c):
    return ((x * 2 + zl) * 4 + y) * 2 + c


def reduce_kernel(
    x_hbm, cot_hbm, gate_hbm, down_hbm, up_hbm, mix_hbm, table_hbm, left_hbm, right_hbm, out_ref,
    wbuf, xv, lv, gcol, pacc, sigp, sigr, xp, acc,
    s1send, s1rel, s1recv, s2f, s2send, s2recv, zf, zsend, zrecv, zag, stage, arecv, factors, gtv, norms, results, gate_ref, mix_ref, table_ref,
    ld, wsend, w1r, st1r, st2r, zp1, zp2, ddr, xr, gsend, gdr, s1relr, s1r, s2r, zr, zagr, asend, ar,
):
    r = lax.axis_index("rep")
    o = lax.axis_index("own")
    c = lax.rem(o, 2)
    y = lax.rem(o // 2, 4)
    zl = lax.rem(o // 8, 2)
    x = o // 16
    z = r * 2 + zl
    m = (x * 4 + y) * 2 + c
    sgn = 2 * zl - 1
    partner = (r, own_of(x, zl, y, 1 - c))

    xs = [lax.rem(x + d, 4) for d in range(4)]
    ys = [lax.rem(y + d, 4) for d in range(4)]
    cs = [c, 1 - c]
    x_part = [v * 16 + zl * 8 for v in xs]
    y_part = [v * 2 for v in ys]
    zs = [lax.rem(z + d, 8) for d in range(8)]

    def along(axis, d):
        if axis == 0:
            return (r, x_part[d % 4] + y_part[0] + c)
        return (r, x_part[0] + y_part[d % 4] + c)

    def zpeer(d):
        zz = zs[d % 8]
        return (lax.div(zz, 2), x * 16 + lax.rem(zz, 2) * 8 + y_part[0] + c)

    def plane(dx, dy, dc):
        return (r, x_part[dx % 4] + y_part[dy % 4] + cs[dc])

    def place(dx, dy, dc):
        return xs[dx % 4] * 8 + y_part[dy % 4] + cs[dc]

    def length(d):
        return min(d, 4 - d)

    offsets = [(dx, dy, dc) for dx in range(4) for dy in range(4) for dc in range(2)][1:]
    offsets.sort(key=lambda t: -(length(t[0]) + length(t[1])))

    quarter = [r, lax.rem(r + sgn + 4, 4), lax.rem(r - sgn + 4, 4), lax.rem(r + 2, 4)]

    pending = []

    def send(src, dst, ssem, rsem, dev):
        cp = pltpu.make_async_remote_copy(
            src_ref=src, dst_ref=dst, send_sem=ssem, recv_sem=rsem,
            device_id=dev, device_id_type=MESH,
        )
        cp.start()
        pending.append(cp)

    def arrived(dst, rsem, dev):
        pltpu.make_async_remote_copy(
            src_ref=dst, dst_ref=dst, send_sem=rsem, recv_sem=rsem,
            device_id=dev, device_id_type=MESH,
        ).wait_recv()

    loads = [
        pltpu.make_async_copy(down_hbm, wbuf.at[0, 0], ld.at[0]),
        pltpu.make_async_copy(up_hbm, wbuf.at[0, 1], ld.at[1]),
    ]
    for s in range(4):
        cols = pl.ds(pl.multiple_of(quarter[s] * 2048, 2048), 2048)
        loads.append(pltpu.make_async_copy(x_hbm.at[:, cols], xv.at[:, cols], ld.at[2 + 2 * s]))
        loads.append(pltpu.make_async_copy(cot_hbm.at[:, cols], lv.at[:, cols], ld.at[3 + 2 * s]))
    loads.append(pltpu.make_async_copy(left_hbm, factors.at[pl.ds(0, 1)], ld.at[10]))
    loads.append(pltpu.make_async_copy(right_hbm, factors.at[pl.ds(1, 1)], ld.at[11]))
    loads.append(pltpu.make_async_copy(gate_hbm, gate_ref, ld.at[12]))
    loads.append(pltpu.make_async_copy(mix_hbm, mix_ref, ld.at[13]))
    loads.append(pltpu.make_async_copy(table_hbm, table_ref, ld.at[14]))
    for cp in loads:
        cp.start()

    barrier = pltpu.get_barrier_semaphore()

    for d in (4, 3, 5):
        pl.semaphore_signal(barrier, inc=1, device_id=zpeer(d), device_id_type=MESH)
    for off in offsets:
        pl.semaphore_signal(barrier, inc=1, device_id=plane(*off), device_id_type=MESH)
    for d in (2, 6, 1, 7):
        pl.semaphore_signal(barrier, inc=1, device_id=zpeer(d), device_id_type=MESH)
    pl.semaphore_wait(barrier, 38)

    pos = (x, y)
    nws = [0]

    def wsem():
        nws[0] += 1
        return wsend.at[nws[0] - 1]

    def unit(s, k):
        return 32 if s == 3 else 16

    def base(s, cc, k):
        return cc * 1024 + (16 * unit(s, 0) if k else 0)

    def piece(s, k, p1, p2):
        u = unit(s, k)
        return pl.ds(pl.multiple_of(base(s, c, k) + (p2 * 4 + p1) * u, u), u)

    def group(s, k, p2):
        u = 4 * unit(s, k)
        return pl.ds(pl.multiple_of(base(s, c, k) + p2 * u, u), u)

    def straight(cc, n):
        size = 128 if n < 3 else 64
        start = 512 + 128 * min(n, 3) + 64 * max(n - 3, 0)
        return pl.ds(pl.multiple_of(cc * 1024 + start, 64), size)

    def p12(k):
        return (pos[0], pos[1]) if k == 0 else (pos[1], pos[0])

    def near(p, d):
        return lax.rem(p + d + 4, 4)

    loads[0].wait()
    loads[1].wait()
    zdest = [
        (lax.rem(r + sgn + 4, 4), own_of(x, 1 - zl, y, c)),
        (lax.rem(r + sgn + 4, 4), own_of(x, zl, y, c)),
        (lax.rem(r + 2, 4), own_of(x, 1 - zl, y, c)),
    ]
    for s in (1, 3, 2):
        for k in range(2):
            rows = piece(s, k, *p12(k))
            send(
                wbuf.at[0, :, rows, :], wbuf.at[s, :, rows, :],
                wsem(), w1r.at[s - 1, k], zdest[s - 1],
            )
    for n in range(5):
        rows = straight(c, n)
        send(wbuf.at[0, :, rows, :], wbuf.at[1, :, rows, :], wsem(), zp1.at[n], zdest[0])
    pair = (r, own_of(x, 1 - zl, y, c))

    def pass_on(n):
        rows = straight(c, n)
        arrived(wbuf.at[1, :, rows, :], zp1.at[n], pair)
        send(wbuf.at[1, :, rows, :], wbuf.at[2, :, rows, :], wsem(), zp2.at[n], pair)

    def rows_at(s, k, stg, d):
        p1, p2 = p12(k)
        return piece(s, k, near(p1, d), p2) if stg == 1 else group(s, k, near(p2, d))

    def s1(s):
        for k in range(2):
            rows = rows_at(s, k, 1, 0)
            arrived(wbuf.at[s, :, rows, :], w1r.at[s - 1, k], zpeer(1))
            for d in (2, 1, 3):
                send(
                    wbuf.at[s, :, rows, :], wbuf.at[s, :, rows, :],
                    wsem(), st1r.at[s - 1, k, d], along(k, d),
                )

    def s2(s):
        for k in range(2):
            for d in (1, 3, 2):
                arrived(wbuf.at[s, :, rows_at(s, k, 1, -d), :], st1r.at[s - 1, k, d], along(k, -d))
        for k in range(2):
            rows = rows_at(s, k, 2, 0)
            for i, d in enumerate((1, 3)):
                send(
                    wbuf.at[s, :, rows, :], wbuf.at[s, :, rows, :],
                    wsem(), st2r.at[s - 1, k, i], along(1 - k, d),
                )

    def f2(s):
        for k in range(2):
            for i, d in enumerate((1, 3)):
                rows = rows_at(s, k, 2, -d)
                arrived(wbuf.at[s, :, rows, :], st2r.at[s - 1, k, i], along(1 - k, -d))
                send(
                    wbuf.at[s, i, rows, :], wbuf.at[s, i, rows, :],
                    wsem(), st2r.at[s - 1, k, 2 + i], along(1 - k, d),
                )

    def stage_far(s, k):
        rows = rows_at(s, k, 2, 2)
        for i, d in enumerate((1, 3)):
            arrived(wbuf.at[s, i, rows, :], st2r.at[s - 1, k, 2 + i], along(1 - k, -d))

    def to_partner(s, rows, i):
        send(wbuf.at[s, :, rows, :], wbuf.at[s, :, rows, :], wsem(), ddr.at[i], partner)

    def gathered(cc):
        return pl.ds(pl.multiple_of(cc * 1024, 512), 512)

    def d2d(s):
        for k in range(2):
            stage_far(s, k)
        to_partner(s, gathered(c), s - 1)

    def d2d_straight1():
        to_partner(1, pl.ds(pl.multiple_of(c * 1024 + 512, 512), 512), 2)

    def d2d_straight2(n):
        arrived(wbuf.at[2, :, straight(c, n), :], zp2.at[n], pair)
        to_partner(2, straight(c, n), 3 + n)

    def d2d_last(far):
        for k in range(2):
            if far:
                stage_far(3, k)
            for i, d in ((3, 2),) if far else ((0, 0), (1, -1), (2, 1)):
                to_partner(3, rows_at(3, k, 2, d), 8 + k * 4 + i)

    def from_partner(s):
        if s < 3:
            arrived(wbuf.at[s, :, gathered(1 - c), :], ddr.at[s - 1], partner)
        if s == 2:
            matmul(2, 1 - c, 0, 1)
        if s == 1:
            rows = pl.ds(pl.multiple_of((1 - c) * 1024 + 512, 512), 512)
            arrived(wbuf.at[1, :, rows, :], ddr.at[2], partner)
        if s == 2:
            for n in range(5):
                arrived(wbuf.at[2, :, straight(1 - c, n), :], ddr.at[3 + n], partner)
        if s == 3:
            for k in range(2):
                for i, d in enumerate((0, -1, 1, 2)):
                    _, p2 = p12(k)
                    rows = pl.ds(
                        pl.multiple_of(base(3, 1 - c, k) + near(p2, d) * 128, 128), 128
                    )
                    arrived(wbuf.at[3, :, rows, :], ddr.at[8 + k * 4 + i], partner)
        matmul(s, 1 - c, 1 if s == 2 else 0, 2)

    def cols_of(s):
        return pl.ds(pl.multiple_of(quarter[s] * 2048, 2048), 2048)

    def share(s):
        loads[2 + 2 * s].wait()
        send(xv.at[:, cols_of(s)], xp.at[:, cols_of(s)], wsem(), xr.at[s], partner)

    def lift(s, first, last):
        if first == 0:
            loads[3 + 2 * s].wait()

        def body(i, carry):
            cols = pl.ds(pl.multiple_of(quarter[s] * 2048 + i * 128, 128), 128)
            g = gcol[...]
            lv[:, cols] = (g * xv[:, cols].astype(F32) * lv[:, cols].astype(F32)).astype(BF16)
            return carry

        lax.fori_loop(first, last, body, 0)

    def matmul(s, cc, first=0, last=2):
        def body(i, carry):
            start = cc * 1024 + i * 512
            rows = pl.ds(pl.multiple_of(start, 512), 512)
            cols = pl.ds(pl.multiple_of(quarter[s] * 2048 + start, 512), 512)
            pacc[0] += jnp.dot(xv[:, cols], wbuf[s, 0, rows, :], preferred_element_type=F32)
            pacc[1] += jnp.dot(lv[:, cols], wbuf[s, 1, rows, :], preferred_element_type=F32)
            return carry

        lax.fori_loop(first, last, body, 0)

    loads[12].wait()
    gcol[...] = jnp.transpose(jnp.broadcast_to(gate_ref[...], (128, 256)))
    pacc[...] = jnp.zeros_like(pacc)
    for s in range(4):
        share(s)
    lift(0, 0, 8)
    s1(1)
    s1(2)
    lift(0, 8, 16)
    s1(3)
    s2(1)
    s2(2)
    pass_on(0)
    lift(1, 0, 8)
    s2(3)
    pass_on(1)
    f2(1)
    lift(1, 8, 16)
    pass_on(2)
    f2(2)
    matmul(0, c)
    pass_on(3)
    lift(2, 0, 8)
    f2(3)
    d2d_last(False)
    d2d_straight2(0)
    pass_on(4)
    d2d_straight1()
    d2d(1)
    lift(2, 8, 16)
    d2d_straight2(1)
    d2d(2)
    lift(3, 0, 16)
    matmul(0, 1 - c)
    matmul(1, c)
    d2d_straight2(2)
    d2d_last(True)
    matmul(3, c)
    from_partner(1)
    d2d_straight2(3)
    from_partner(3)
    d2d_straight2(4)
    matmul(2, c)
    from_partner(2)

    loads[13].wait()
    loads[14].wait()
    inner = jnp.tanh(pacc[0]).astype(BF16)
    outer = jnp.tanh(jnp.dot(inner, mix_ref[...], preferred_element_type=F32))
    slope = (pacc[1] * (1.0 - outer * outer)).astype(BF16)
    through = lax.dot_general(
        slope, mix_ref[...], (((1,), (1,)), ((), ())), preferred_element_type=F32
    )
    inner_wide = inner.astype(F32)
    signal = through * (1.0 - inner_wide * inner_wide)
    sigp[...] = jnp.transpose(signal).astype(BF16)
    other_rows = pl.ds(pl.multiple_of((1 - c) * 128, 128), 128)
    own_rows = pl.ds(pl.multiple_of(c * 128, 128), 128)

    ngs = [0]

    def gsem():
        ngs[0] += 1
        return gsend.at[ngs[0] - 1]

    send(sigp.at[other_rows], sigr, gsem(), gdr, partner)

    def own_tokens(i, carry):
        cols = pl.ds(pl.multiple_of(i * 256, 256), 256)
        acc[i] = jnp.dot(sigp[own_rows, :], xv[:, cols], preferred_element_type=F32)
        return carry

    lax.fori_loop(0, 32, own_tokens, 0, unroll=4)
    for s in range(4):
        arrived(xp.at[:, cols_of(s)], xr.at[s], partner)
    arrived(sigr, gdr, partner)

    def rows16(k, d):
        i = near(pos[k], d)
        return pl.ds(pl.multiple_of(k * 64 + i * 16, 16), 16)

    def merge(g):
        role, d = (2, -1) if g % 2 == 0 else (1, 1)

        def body(i, carry):
            b = g * 8 + i
            cols = pl.ds(pl.multiple_of(b * 256, 256), 256)
            acc[b] += jnp.dot(sigr[...], xp[:, cols], preferred_element_type=F32)
            for k in range(2):
                s1send[k, 0, b] = acc[b, rows16(k, 2), :].astype(BF16)
                s1send[k, role, b] = acc[b, rows16(k, d), :].astype(BF16)
            return carry

        lax.fori_loop(0, 8, body, 0, unroll=4)

    def far_out(g):
        side, rnd = g % 2, g // 2
        blk, rel = pl.ds(g * 8, 8), pl.ds(rnd * 8, 8)
        for k in range(2):
            send(
                s1send.at[k, 0, blk], s1rel.at[k, side, rel], gsem(),
                s1relr.at[k, side, rnd], along(k, 1 - 2 * side),
            )

    def near_out(g, role):
        blk = pl.ds(g * 8, 8)
        for k in range(2):
            send(
                s1send.at[k, role, blk], s1recv.at[k, role - 1, blk], gsem(),
                s1r.at[k, role - 1, g], along(k, 3 - 2 * role),
            )

    def relay(g):
        side, rnd = g % 2, g // 2
        rel = pl.ds(rnd * 8, 8)
        d = 1 - 2 * side
        for k in range(2):
            arrived(s1rel.at[k, side, rel], s1relr.at[k, side, rnd], along(k, -d))

            def body(i, carry, k=k):
                b = g * 8 + i
                s1send[k, 1 + side, b] = (
                    acc[b, rows16(k, d), :] + s1rel[k, side, rnd * 8 + i].astype(F32)
                ).astype(BF16)
                return carry

            lax.fori_loop(0, 8, body, 0, unroll=4)
        near_out(g, 1 + side)

    def finish(rnd):
        half = pl.ds(rnd * 128, 128)
        for k in range(2):
            for role in range(2):
                for g in (2 * rnd, 2 * rnd + 1):
                    arrived(
                        s1recv.at[k, role, pl.ds(g * 8, 8)], s1r.at[k, role, g],
                        along(k, 2 * role - 1),
                    )

            def own_sum(i, carry, k=k):
                tot = []
                for q in range(2):
                    b = i * 2 + q
                    tot.append(
                        acc[b, rows16(k, 0), :]
                        + s1recv[k, 0, b].astype(F32)
                        + s1recv[k, 1, b].astype(F32)
                    )
                rows = pl.ds(pl.multiple_of(i * 16, 16), 16)
                for j in range(4):
                    a, h = j // 2, j % 2
                    part = jnp.concatenate(
                        [t[a * 8 : a * 8 + 8, h * 128 : h * 128 + 128] for t in tot], axis=0
                    )
                    s2f[k, j, rows, :] = part
                    s2send[k, j, rows, :] = part.astype(BF16)
                return carry

            lax.fori_loop(rnd * 8, rnd * 8 + 8, own_sum, 0, unroll=4)
            for d in (2, 1, 3):
                j = near(pos[1 - k], d)
                send(
                    s2send.at[k, j, half], s2recv.at[k, d - 1, half], gsem(),
                    s2r.at[k, d - 1, rnd], along(1 - k, d),
                )

    merge(0)
    far_out(0)
    near_out(0, 2)
    merge(1)
    far_out(1)
    near_out(1, 1)
    merge(2)
    far_out(2)
    merge(3)
    far_out(3)
    relay(0)
    near_out(3, 1)
    relay(1)
    near_out(2, 2)
    relay(2)
    finish(0)
    relay(3)
    finish(1)

    parts = []
    for k in range(2):
        tot = s2f[k, pos[1 - k]]
        for d in (1, 3, 2):
            for rnd in range(2):
                half = pl.ds(rnd * 128, 128)
                arrived(s2recv.at[k, d - 1, half], s2r.at[k, d - 1, rnd], along(1 - k, -d))
            tot = tot + s2recv[k, d - 1].astype(F32)
        parts.append(tot.reshape(32, 8, 128))
    both = jnp.concatenate(parts, axis=1)
    zf[...] = both
    zsend[...] = both.astype(BF16)

    for d in (4, 3, 5, 2, 6, 1, 7):
        zz = lax.rem(z + d, 8)
        send(zsend.at[pl.ds(zz * 4, 4)], zrecv.at[d - 1], gsem(), zr.at[d - 1], zpeer(d))
    tot = zf[pl.ds(z * 4, 4)]
    for d in (1, 7, 2, 6, 3, 5, 4):
        arrived(zrecv.at[d - 1], zr.at[d - 1], zpeer(-d))
        tot = tot + zrecv[d - 1].astype(F32)
    mine = pl.ds(z * 4, 4)
    zag[mine] = tot.astype(BF16)
    for d in (4, 3, 5, 2, 6, 1, 7):
        send(zag.at[mine], zag.at[mine], gsem(), zagr.at[d - 1], zpeer(d))
    for d in (1, 7, 2, 6, 3, 5, 4):
        zz = lax.rem(z - d + 8, 8)
        arrived(zag.at[pl.ds(zz * 4, 4)], zagr.at[d - 1], zpeer(-d))

    for e, off in enumerate(offsets):
        stage[e] = zag[jnp.maximum(table_ref[plane(*off)[1]], 0)]
    arecv[m] = zag[jnp.maximum(table_ref[o], 0)]
    for e, off in enumerate(offsets):
        pltpu.make_async_remote_copy(
            src_ref=stage.at[e], dst_ref=arecv.at[m], send_sem=asend, recv_sem=ar.at[e],
            device_id=plane(*off), device_id_type=MESH,
        ).start()
    for cp in pending:
        cp.wait_send()
    for e, (dx, dy, dc) in reversed(list(enumerate(offsets))):
        arrived(arecv.at[place(-dx, -dy, dc)], ar.at[e], plane(-dx, -dy, dc))
    for xx in range(4):
        for yy in range(4):
            for cc in range(2):
                tile = arecv[(xx * 4 + yy) * 2 + cc]
                r0 = cc * 128 + xx * 16 + (yy // 2) * 8
                l0 = (yy % 2) * 128
                gtv[r0 : r0 + 8, l0 : l0 + 128] = tile[0:8].astype(F32)
                r1 = cc * 128 + 64 + yy * 16 + (xx // 2) * 8
                l1 = (xx % 2) * 128
                gtv[r1 : r1 + 8, l1 : l1 + 128] = tile[8:16].astype(F32)

    first = pl.ds(0, 31)
    pltpu.make_async_remote_copy(
        src_ref=stage.at[first], dst_ref=arecv.at[first], send_sem=asend, recv_sem=asend,
        device_id=partner, device_id_type=MESH,
    ).wait_send()
    loads[10].wait()
    loads[11].wait()
    roots(gtv, factors, norms, results, table_ref[o] >= 0, out_ref)


def reduced_block(inputs, cotangent, gate, down_weight, up_weight, mixing, table, left, right):
    any_spec = pl.BlockSpec(memory_space=pltpu.HBM)
    vm = pl.BlockSpec(memory_space=pltpu.VMEM)
    dma = pltpu.SemaphoreType.DMA
    V = pltpu.VMEM
    return pl.pallas_call(
        reduce_kernel,
        name="reduce",
        out_shape=jax.ShapeDtypeStruct((256, 256), F32),
        in_specs=[any_spec] * 9,
        out_specs=vm,
        scratch_shapes=[
            V((4, 2, 2048, 256), BF16),
            V((256, 8192), BF16),
            V((256, 8192), BF16),
            V((256, 128), F32),
            V((2, 256, 256), F32),
            V((256, 256), BF16),
            V((128, 256), BF16),
            V((256, 8192), BF16),
            V((32, 128, 256), F32),
            V((2, 3, 32, 16, 256), BF16),
            V((2, 2, 16, 16, 256), BF16),
            V((2, 2, 32, 16, 256), BF16),
            V((2, 4, 256, 128), F32),
            V((2, 4, 256, 128), BF16),
            V((2, 3, 256, 128), BF16),
            V((32, 16, 128), F32),
            V((32, 16, 128), BF16),
            V((7, 4, 16, 128), BF16),
            V((32, 16, 128), BF16),
            V((32, 16, 128), BF16),
            V((32, 16, 128), BF16),
            V((2, R, R), F32),
            V((R, R), F32),
            V((2, R, R), F32),
            V((2, R, R), F32),
            V((1, 256), F32),
            V((R, R), BF16),
            pltpu.SMEM((64,), jnp.int32),
            dma((15,)),
            dma((97,)),
            dma((3, 2)),
            dma((3, 2, 4)),
            dma((3, 2, 4)),
            dma((5,)),
            dma((5,)),
            dma((16,)),
            dma((4,)),
            dma((54,)),
            dma,
            dma((2, 2, 2)),
            dma((2, 2, 4)),
            dma((2, 3, 2)),
            dma((7,)),
            dma((7,)),
            dma,
            dma((31,)),
        ],
        compiler_params=pltpu.CompilerParams(
            collective_id=0, has_side_effects=True, vmem_limit_bytes=63 * 1024 * 1024
        ),
    )(inputs, cotangent, gate, down_weight, up_weight, mixing, table, left, right)


def halves(a):
    hi = a.astype(BF16)
    return hi, (a - hi.astype(F32)).astype(BF16)


def dot(a, b):
    return jnp.dot(a, b, preferred_element_type=F32)


def product(a, b):
    (ah, al), (bh, bl) = a, b
    lhs = jnp.concatenate([ah, ah, al], axis=1)
    rhs = jnp.concatenate([bh, bl, bh], axis=0)
    return dot(lhs, rhs)


def roots(gt_ref, factors, norms, results, filled, out_ref):
    eye = (
        lax.broadcasted_iota(jnp.int32, (R, R), 0) == lax.broadcasted_iota(jnp.int32, (R, R), 1)
    ).astype(F32)
    scaled = gt_ref[...] * (1.0 / TOKENS)
    gt = scaled.astype(BF16)
    g = jnp.transpose(scaled).astype(BF16)
    news = [
        BETA * factors[0] + (1.0 - BETA) * dot(g, gt),
        BETA * factors[1] + (1.0 - BETA) * dot(gt, g),
    ]
    for i, a in enumerate(news):
        shifted = a + EPS * eye
        norm = jnp.sqrt(jnp.sum(shifted * shifted, keepdims=True))
        m = shifted / norm
        results[i] = lax.rsqrt(jnp.sqrt(norm)) * ((5.0 * eye - m) / 4.0)
        norms[i] = m

    def advance(m, mb):
        e = dot(mb, mb) * (1.0 / 16.0) - m * (10.0 / 16.0)
        eb = e.astype(BF16)
        h = (25.0 / 8.0) * e + dot(eb, eb)
        return (625.0 / 256.0) * m + dot(h.astype(BF16), mb)

    def multiply(x, mb):
        return 1.25 * x - 0.25 * dot(x.astype(BF16), mb)

    for i in range(2):
        norms[i] = advance(norms[i], norms[i].astype(BF16))

    def sweep(step, carry):
        for i in range(2):
            m = norms[i]
            mb = m.astype(BF16)
            results[i] = multiply(results[i], mb)
            norms[i] = advance(m, mb)
        return carry

    lax.fori_loop(0, ITERS - 2, sweep, 0, unroll=True)
    left, right = [multiply(results[i], norms[i].astype(BF16)) for i in range(2)]
    half = dot(jnp.concatenate(halves(left), axis=1), jnp.concatenate([g, g], axis=0))
    done = product(halves(half), halves(right))
    out_ref[...] = jnp.where(filled, done, 0.0)


def shards(
    inputs, cotangent, gate, down_weight, up_weight, mixing, owner_table, left_factor, right_factor
):
    table = owner_table.reshape(-1)
    return reduced_block(
        inputs, cotangent, gate.reshape(1, -1), down_weight, up_weight, mixing, table,
        left_factor, right_factor,
    )


def solution(mesh):
    in_specs = (
        P(("rep", "own"), None),
        P(("rep", "own"), None),
        P(("rep", "own")),
        P("rep", None),
        P("rep", None),
        P(),
        P(),
        P("own", None, None),
        P("own", None, None),
    )
    return jax.shard_map(
        shards, mesh=mesh, in_specs=in_specs, out_specs=P("own", None), check_vma=False
    )
```

```python
import functools

import jax
import jax.numpy as jnp
from jax import lax
from jax.experimental import pallas as pl
from jax.experimental.pallas import tpu as pltpu
from jax.sharding import PartitionSpec as P

R = 256
ITERS = 5
BETA = 0.95
EPS = 1e-06
TOKENS = 65536

F32 = jnp.float32
BF16 = jnp.bfloat16
MESH = pl.DeviceIdType.MESH


def own_of(x, zl, y, c):
    return ((x * 2 + zl) * 4 + y) * 2 + c


def reduce_kernel(
    x_hbm, cot_hbm, gate_hbm, down_hbm, up_hbm, mix_hbm, table_hbm, left_hbm, right_hbm, out_ref,
    wbuf, xv, lv, gcol, pacc, sigp, sigr, xp, acc,
    s1send, s1rel, s1recv, s2f, s2send, s2recv, zf, zsend, zrecv, zag, stage, arecv, factors, gtv, norms, results, gate_ref, mix_ref, table_ref,
    ld, wsend, w1r, st1r, st2r, zp1, zp2, ddr, xr, gsend, gdr, s1relr, s1r, s2r, zr, zagr, asend, ar,
):
    r = lax.axis_index("rep")
    o = lax.axis_index("own")
    c = lax.rem(o, 2)
    y = lax.rem(o // 2, 4)
    zl = lax.rem(o // 8, 2)
    x = o // 16
    z = r * 2 + zl
    m = (x * 4 + y) * 2 + c
    sgn = 2 * zl - 1
    partner = (r, own_of(x, zl, y, 1 - c))

    xs = [lax.rem(x + d, 4) for d in range(4)]
    ys = [lax.rem(y + d, 4) for d in range(4)]
    cs = [c, 1 - c]
    x_part = [v * 16 + zl * 8 for v in xs]
    y_part = [v * 2 for v in ys]
    zs = [lax.rem(z + d, 8) for d in range(8)]

    def along(axis, d):
        if axis == 0:
            return (r, x_part[d % 4] + y_part[0] + c)
        return (r, x_part[0] + y_part[d % 4] + c)

    def zpeer(d):
        zz = zs[d % 8]
        return (lax.div(zz, 2), x * 16 + lax.rem(zz, 2) * 8 + y_part[0] + c)

    def plane(dx, dy, dc):
        return (r, x_part[dx % 4] + y_part[dy % 4] + cs[dc])

    def place(dx, dy, dc):
        return xs[dx % 4] * 8 + y_part[dy % 4] + cs[dc]

    def length(d):
        return min(d, 4 - d)

    offsets = [(dx, dy, dc) for dx in range(4) for dy in range(4) for dc in range(2)][1:]
    offsets.sort(key=lambda t: -(length(t[0]) + length(t[1])))

    quarter = [r, lax.rem(r + sgn + 4, 4), lax.rem(r - sgn + 4, 4), lax.rem(r + 2, 4)]

    pending = []

    def send(src, dst, ssem, rsem, dev):
        cp = pltpu.make_async_remote_copy(
            src_ref=src, dst_ref=dst, send_sem=ssem, recv_sem=rsem,
            device_id=dev, device_id_type=MESH,
        )
        cp.start()
        pending.append(cp)

    def arrived(dst, rsem, dev):
        pltpu.make_async_remote_copy(
            src_ref=dst, dst_ref=dst, send_sem=rsem, recv_sem=rsem,
            device_id=dev, device_id_type=MESH,
        ).wait_recv()

    loads = [
        pltpu.make_async_copy(down_hbm, wbuf.at[0, 0], ld.at[0]),
        pltpu.make_async_copy(up_hbm, wbuf.at[0, 1], ld.at[1]),
    ]
    for s in range(4):
        cols = pl.ds(pl.multiple_of(quarter[s] * 2048, 2048), 2048)
        loads.append(pltpu.make_async_copy(x_hbm.at[:, cols], xv.at[:, cols], ld.at[2 + 2 * s]))
        loads.append(pltpu.make_async_copy(cot_hbm.at[:, cols], lv.at[:, cols], ld.at[3 + 2 * s]))
    loads.append(pltpu.make_async_copy(left_hbm, factors.at[pl.ds(0, 1)], ld.at[10]))
    loads.append(pltpu.make_async_copy(right_hbm, factors.at[pl.ds(1, 1)], ld.at[11]))
    loads.append(pltpu.make_async_copy(gate_hbm, gate_ref, ld.at[12]))
    loads.append(pltpu.make_async_copy(mix_hbm, mix_ref, ld.at[13]))
    loads.append(pltpu.make_async_copy(table_hbm, table_ref, ld.at[14]))
    for cp in loads:
        cp.start()

    barrier = pltpu.get_barrier_semaphore()

    for d in (4, 3, 5):
        pl.semaphore_signal(barrier, inc=1, device_id=zpeer(d), device_id_type=MESH)
    for off in offsets:
        pl.semaphore_signal(barrier, inc=1, device_id=plane(*off), device_id_type=MESH)
    for d in (2, 6, 1, 7):
        pl.semaphore_signal(barrier, inc=1, device_id=zpeer(d), device_id_type=MESH)
    pl.semaphore_wait(barrier, 38)

    pos = (x, y)
    nws = [0]

    def wsem():
        nws[0] += 1
        return wsend.at[nws[0] - 1]

    def unit(s, k):
        return 32 if s == 3 else 16

    def base(s, cc, k):
        return cc * 1024 + (16 * unit(s, 0) if k else 0)

    def piece(s, k, p1, p2):
        u = unit(s, k)
        return pl.ds(pl.multiple_of(base(s, c, k) + (p2 * 4 + p1) * u, u), u)

    def group(s, k, p2):
        u = 4 * unit(s, k)
        return pl.ds(pl.multiple_of(base(s, c, k) + p2 * u, u), u)

    def straight(cc, n):
        size = 128 if n < 3 else 64
        start = 512 + 128 * min(n, 3) + 64 * max(n - 3, 0)
        return pl.ds(pl.multiple_of(cc * 1024 + start, 64), size)

    def p12(k):
        return (pos[0], pos[1]) if k == 0 else (pos[1], pos[0])

    def near(p, d):
        return lax.rem(p + d + 4, 4)

    loads[0].wait()
    loads[1].wait()
    zdest = [
        (lax.rem(r + sgn + 4, 4), own_of(x, 1 - zl, y, c)),
        (lax.rem(r + sgn + 4, 4), own_of(x, zl, y, c)),
        (lax.rem(r + 2, 4), own_of(x, 1 - zl, y, c)),
    ]
    for s in (1, 3, 2):
        for k in range(2):
            rows = piece(s, k, *p12(k))
            send(
                wbuf.at[0, :, rows, :], wbuf.at[s, :, rows, :],
                wsem(), w1r.at[s - 1, k], zdest[s - 1],
            )
    for n in range(5):
        rows = straight(c, n)
        send(wbuf.at[0, :, rows, :], wbuf.at[1, :, rows, :], wsem(), zp1.at[n], zdest[0])
    pair = (r, own_of(x, 1 - zl, y, c))

    def pass_on(n):
        rows = straight(c, n)
        arrived(wbuf.at[1, :, rows, :], zp1.at[n], pair)
        send(wbuf.at[1, :, rows, :], wbuf.at[2, :, rows, :], wsem(), zp2.at[n], pair)

    def rows_at(s, k, stg, d):
        p1, p2 = p12(k)
        return piece(s, k, near(p1, d), p2) if stg == 1 else group(s, k, near(p2, d))

    def s1(s):
        for k in range(2):
            rows = rows_at(s, k, 1, 0)
            arrived(wbuf.at[s, :, rows, :], w1r.at[s - 1, k], zpeer(1))
            for d in (2, 1, 3):
                send(
                    wbuf.at[s, :, rows, :], wbuf.at[s, :, rows, :],
                    wsem(), st1r.at[s - 1, k, d], along(k, d),
                )

    def s2(s):
        for k in range(2):
            for d in (1, 3, 2):
                arrived(wbuf.at[s, :, rows_at(s, k, 1, -d), :], st1r.at[s - 1, k, d], along(k, -d))
        for k in range(2):
            rows = rows_at(s, k, 2, 0)
            for i, d in enumerate((1, 3)):
                send(
                    wbuf.at[s, :, rows, :], wbuf.at[s, :, rows, :],
                    wsem(), st2r.at[s - 1, k, i], along(1 - k, d),
                )

    def f2(s):
        for k in range(2):
            for i, d in enumerate((1, 3)):
                rows = rows_at(s, k, 2, -d)
                arrived(wbuf.at[s, :, rows, :], st2r.at[s - 1, k, i], along(1 - k, -d))
                send(
                    wbuf.at[s, i, rows, :], wbuf.at[s, i, rows, :],
                    wsem(), st2r.at[s - 1, k, 2 + i], along(1 - k, d),
                )

    def stage_far(s, k):
        rows = rows_at(s, k, 2, 2)
        for i, d in enumerate((1, 3)):
            arrived(wbuf.at[s, i, rows, :], st2r.at[s - 1, k, 2 + i], along(1 - k, -d))

    def to_partner(s, rows, i):
        send(wbuf.at[s, :, rows, :], wbuf.at[s, :, rows, :], wsem(), ddr.at[i], partner)

    def gathered(cc):
        return pl.ds(pl.multiple_of(cc * 1024, 512), 512)

    def d2d(s):
        for k in range(2):
            stage_far(s, k)
        to_partner(s, gathered(c), s - 1)

    def d2d_straight1():
        to_partner(1, pl.ds(pl.multiple_of(c * 1024 + 512, 512), 512), 2)

    def d2d_straight2(n):
        arrived(wbuf.at[2, :, straight(c, n), :], zp2.at[n], pair)
        to_partner(2, straight(c, n), 3 + n)

    def d2d_last(far):
        for k in range(2):
            if far:
                stage_far(3, k)
            for i, d in ((3, 2),) if far else ((0, 0), (1, -1), (2, 1)):
                to_partner(3, rows_at(3, k, 2, d), 8 + k * 4 + i)

    def from_partner(s):
        if s < 3:
            arrived(wbuf.at[s, :, gathered(1 - c), :], ddr.at[s - 1], partner)
        if s == 2:
            matmul(2, 1 - c, 0, 1)
        if s == 1:
            rows = pl.ds(pl.multiple_of((1 - c) * 1024 + 512, 512), 512)
            arrived(wbuf.at[1, :, rows, :], ddr.at[2], partner)
        if s == 2:
            for n in range(5):
                arrived(wbuf.at[2, :, straight(1 - c, n), :], ddr.at[3 + n], partner)
        if s == 3:
            for k in range(2):
                for i, d in enumerate((0, -1, 1, 2)):
                    _, p2 = p12(k)
                    rows = pl.ds(
                        pl.multiple_of(base(3, 1 - c, k) + near(p2, d) * 128, 128), 128
                    )
                    arrived(wbuf.at[3, :, rows, :], ddr.at[8 + k * 4 + i], partner)
        matmul(s, 1 - c, 1 if s == 2 else 0, 2)

    def cols_of(s):
        return pl.ds(pl.multiple_of(quarter[s] * 2048, 2048), 2048)

    def share(s):
        loads[2 + 2 * s].wait()
        send(xv.at[:, cols_of(s)], xp.at[:, cols_of(s)], wsem(), xr.at[s], partner)

    def lift(s, first, last):
        if first == 0:
            loads[3 + 2 * s].wait()

        def body(i, carry):
            cols = pl.ds(pl.multiple_of(quarter[s] * 2048 + i * 128, 128), 128)
            g = gcol[...]
            lv[:, cols] = (g * xv[:, cols].astype(F32) * lv[:, cols].astype(F32)).astype(BF16)
            return carry

        lax.fori_loop(first, last, body, 0)

    def matmul(s, cc, first=0, last=2):
        def body(i, carry):
            start = cc * 1024 + i * 512
            rows = pl.ds(pl.multiple_of(start, 512), 512)
            cols = pl.ds(pl.multiple_of(quarter[s] * 2048 + start, 512), 512)
            pacc[0] += jnp.dot(xv[:, cols], wbuf[s, 0, rows, :], preferred_element_type=F32)
            pacc[1] += jnp.dot(lv[:, cols], wbuf[s, 1, rows, :], preferred_element_type=F32)
            return carry

        lax.fori_loop(first, last, body, 0)

    loads[12].wait()
    gcol[...] = jnp.transpose(jnp.broadcast_to(gate_ref[...], (128, 256)))
    pacc[...] = jnp.zeros_like(pacc)
    for s in range(4):
        share(s)
    lift(0, 0, 8)
    s1(1)
    s1(2)
    lift(0, 8, 16)
    s1(3)
    s2(1)
    s2(2)
    pass_on(0)
    lift(1, 0, 8)
    s2(3)
    pass_on(1)
    f2(1)
    lift(1, 8, 16)
    pass_on(2)
    f2(2)
    matmul(0, c)
    pass_on(3)
    lift(2, 0, 8)
    f2(3)
    d2d_last(False)
    d2d_straight2(0)
    pass_on(4)
    d2d_straight1()
    d2d(1)
    lift(2, 8, 16)
    d2d_straight2(1)
    d2d(2)
    lift(3, 0, 16)
    matmul(0, 1 - c)
    matmul(1, c)
    d2d_straight2(2)
    d2d_last(True)
    matmul(3, c)
    from_partner(1)
    d2d_straight2(3)
    from_partner(3)
    d2d_straight2(4)
    matmul(2, c)
    from_partner(2)

    loads[13].wait()
    loads[14].wait()
    inner = jnp.tanh(pacc[0]).astype(BF16)
    outer = jnp.tanh(jnp.dot(inner, mix_ref[...], preferred_element_type=F32))
    slope = (pacc[1] * (1.0 - outer * outer)).astype(BF16)
    through = lax.dot_general(
        slope, mix_ref[...], (((1,), (1,)), ((), ())), preferred_element_type=F32
    )
    inner_wide = inner.astype(F32)
    signal = through * (1.0 - inner_wide * inner_wide)
    sigp[...] = jnp.transpose(signal).astype(BF16)
    other_rows = pl.ds(pl.multiple_of((1 - c) * 128, 128), 128)
    own_rows = pl.ds(pl.multiple_of(c * 128, 128), 128)

    ngs = [0]

    def gsem():
        ngs[0] += 1
        return gsend.at[ngs[0] - 1]

    send(sigp.at[other_rows], sigr, gsem(), gdr, partner)

    def own_tokens(i, carry):
        cols = pl.ds(pl.multiple_of(i * 256, 256), 256)
        acc[i] = jnp.dot(sigp[own_rows, :], xv[:, cols], preferred_element_type=F32)
        return carry

    lax.fori_loop(0, 32, own_tokens, 0, unroll=8)
    for s in range(4):
        arrived(xp.at[:, cols_of(s)], xr.at[s], partner)
    arrived(sigr, gdr, partner)

    def rows16(k, d):
        i = near(pos[k], d)
        return pl.ds(pl.multiple_of(k * 64 + i * 16, 16), 16)

    def merge(g):
        role, d = (2, -1) if g % 2 == 0 else (1, 1)

        def body(i, carry):
            b = g * 8 + i
            cols = pl.ds(pl.multiple_of(b * 256, 256), 256)
            acc[b] += jnp.dot(sigr[...], xp[:, cols], preferred_element_type=F32)
            for k in range(2):
                s1send[k, 0, b] = acc[b, rows16(k, 2), :].astype(BF16)
                s1send[k, role, b] = acc[b, rows16(k, d), :].astype(BF16)
            return carry

        lax.fori_loop(0, 8, body, 0, unroll=4)

    def far_out(g):
        side, rnd = g % 2, g // 2
        blk, rel = pl.ds(g * 8, 8), pl.ds(rnd * 8, 8)
        for k in range(2):
            send(
                s1send.at[k, 0, blk], s1rel.at[k, side, rel], gsem(),
                s1relr.at[k, side, rnd], along(k, 1 - 2 * side),
            )

    def near_out(g, role):
        blk = pl.ds(g * 8, 8)
        for k in range(2):
            send(
                s1send.at[k, role, blk], s1recv.at[k, role - 1, blk], gsem(),
                s1r.at[k, role - 1, g], along(k, 3 - 2 * role),
            )

    def relay(g):
        side, rnd = g % 2, g // 2
        rel = pl.ds(rnd * 8, 8)
        d = 1 - 2 * side
        for k in range(2):
            arrived(s1rel.at[k, side, rel], s1relr.at[k, side, rnd], along(k, -d))

            def body(i, carry, k=k):
                b = g * 8 + i
                s1send[k, 1 + side, b] = (
                    acc[b, rows16(k, d), :] + s1rel[k, side, rnd * 8 + i].astype(F32)
                ).astype(BF16)
                return carry

            lax.fori_loop(0, 8, body, 0, unroll=4)
        near_out(g, 1 + side)

    def finish(rnd):
        half = pl.ds(rnd * 128, 128)
        for k in range(2):
            for role in range(2):
                for g in (2 * rnd, 2 * rnd + 1):
                    arrived(
                        s1recv.at[k, role, pl.ds(g * 8, 8)], s1r.at[k, role, g],
                        along(k, 2 * role - 1),
                    )

            def own_sum(i, carry, k=k):
                tot = []
                for q in range(2):
                    b = i * 2 + q
                    tot.append(
                        acc[b, rows16(k, 0), :]
                        + s1recv[k, 0, b].astype(F32)
                        + s1recv[k, 1, b].astype(F32)
                    )
                rows = pl.ds(pl.multiple_of(i * 16, 16), 16)
                for j in range(4):
                    a, h = j // 2, j % 2
                    part = jnp.concatenate(
                        [t[a * 8 : a * 8 + 8, h * 128 : h * 128 + 128] for t in tot], axis=0
                    )
                    s2f[k, j, rows, :] = part
                    s2send[k, j, rows, :] = part.astype(BF16)
                return carry

            lax.fori_loop(rnd * 8, rnd * 8 + 8, own_sum, 0, unroll=4)
            for d in (2, 1, 3):
                j = near(pos[1 - k], d)
                send(
                    s2send.at[k, j, half], s2recv.at[k, d - 1, half], gsem(),
                    s2r.at[k, d - 1, rnd], along(1 - k, d),
                )

    merge(0)
    far_out(0)
    near_out(0, 2)
    merge(1)
    far_out(1)
    near_out(1, 1)
    merge(2)
    far_out(2)
    merge(3)
    far_out(3)
    relay(0)
    near_out(3, 1)
    relay(1)
    near_out(2, 2)
    relay(2)
    finish(0)
    relay(3)
    finish(1)

    parts = []
    for k in range(2):
        tot = s2f[k, pos[1 - k]]
        for d in (1, 3, 2):
            for rnd in range(2):
                half = pl.ds(rnd * 128, 128)
                arrived(s2recv.at[k, d - 1, half], s2r.at[k, d - 1, rnd], along(1 - k, -d))
            tot = tot + s2recv[k, d - 1].astype(F32)
        parts.append(tot.reshape(32, 8, 128))
    both = jnp.concatenate(parts, axis=1)
    zf[...] = both
    zsend[...] = both.astype(BF16)

    for d in (4, 3, 5, 2, 6, 1, 7):
        zz = lax.rem(z + d, 8)
        send(zsend.at[pl.ds(zz * 4, 4)], zrecv.at[d - 1], gsem(), zr.at[d - 1], zpeer(d))
    tot = zf[pl.ds(z * 4, 4)]
    for d in (1, 7, 2, 6, 3, 5, 4):
        arrived(zrecv.at[d - 1], zr.at[d - 1], zpeer(-d))
        tot = tot + zrecv[d - 1].astype(F32)
    mine = pl.ds(z * 4, 4)
    zag[mine] = tot.astype(BF16)
    for d in (4, 3, 5, 2, 6, 1, 7):
        send(zag.at[mine], zag.at[mine], gsem(), zagr.at[d - 1], zpeer(d))
    for d in (1, 7, 2, 6, 3, 5, 4):
        zz = lax.rem(z - d + 8, 8)
        arrived(zag.at[pl.ds(zz * 4, 4)], zagr.at[d - 1], zpeer(-d))

    for e, off in enumerate(offsets):
        stage[e] = zag[jnp.maximum(table_ref[plane(*off)[1]], 0)]
    arecv[m] = zag[jnp.maximum(table_ref[o], 0)]
    for e, off in enumerate(offsets):
        pltpu.make_async_remote_copy(
            src_ref=stage.at[e], dst_ref=arecv.at[m], send_sem=asend, recv_sem=ar.at[e],
            device_id=plane(*off), device_id_type=MESH,
        ).start()
    for cp in pending:
        cp.wait_send()
    for e, (dx, dy, dc) in reversed(list(enumerate(offsets))):
        arrived(arecv.at[place(-dx, -dy, dc)], ar.at[e], plane(-dx, -dy, dc))
    for xx in range(4):
        for yy in range(4):
            for cc in range(2):
                tile = arecv[(xx * 4 + yy) * 2 + cc]
                r0 = cc * 128 + xx * 16 + (yy // 2) * 8
                l0 = (yy % 2) * 128
                gtv[r0 : r0 + 8, l0 : l0 + 128] = tile[0:8].astype(F32)
                r1 = cc * 128 + 64 + yy * 16 + (xx // 2) * 8
                l1 = (xx % 2) * 128
                gtv[r1 : r1 + 8, l1 : l1 + 128] = tile[8:16].astype(F32)

    first = pl.ds(0, 31)
    pltpu.make_async_remote_copy(
        src_ref=stage.at[first], dst_ref=arecv.at[first], send_sem=asend, recv_sem=asend,
        device_id=partner, device_id_type=MESH,
    ).wait_send()
    loads[10].wait()
    loads[11].wait()
    roots(gtv, factors, norms, results, table_ref[o] >= 0, out_ref)


def reduced_block(inputs, cotangent, gate, down_weight, up_weight, mixing, table, left, right):
    any_spec = pl.BlockSpec(memory_space=pltpu.HBM)
    vm = pl.BlockSpec(memory_space=pltpu.VMEM)
    dma = pltpu.SemaphoreType.DMA
    V = pltpu.VMEM
    return pl.pallas_call(
        reduce_kernel,
        name="reduce",
        out_shape=jax.ShapeDtypeStruct((256, 256), F32),
        in_specs=[any_spec] * 9,
        out_specs=vm,
        scratch_shapes=[
            V((4, 2, 2048, 256), BF16),
            V((256, 8192), BF16),
            V((256, 8192), BF16),
            V((256, 128), F32),
            V((2, 256, 256), F32),
            V((256, 256), BF16),
            V((128, 256), BF16),
            V((256, 8192), BF16),
            V((32, 128, 256), F32),
            V((2, 3, 32, 16, 256), BF16),
            V((2, 2, 16, 16, 256), BF16),
            V((2, 2, 32, 16, 256), BF16),
            V((2, 4, 256, 128), F32),
            V((2, 4, 256, 128), BF16),
            V((2, 3, 256, 128), BF16),
            V((32, 16, 128), F32),
            V((32, 16, 128), BF16),
            V((7, 4, 16, 128), BF16),
            V((32, 16, 128), BF16),
            V((32, 16, 128), BF16),
            V((32, 16, 128), BF16),
            V((2, R, R), F32),
            V((R, R), F32),
            V((2, R, R), F32),
            V((2, R, R), F32),
            V((1, 256), F32),
            V((R, R), BF16),
            pltpu.SMEM((64,), jnp.int32),
            dma((15,)),
            dma((97,)),
            dma((3, 2)),
            dma((3, 2, 4)),
            dma((3, 2, 4)),
            dma((5,)),
            dma((5,)),
            dma((16,)),
            dma((4,)),
            dma((54,)),
            dma,
            dma((2, 2, 2)),
            dma((2, 2, 4)),
            dma((2, 3, 2)),
            dma((7,)),
            dma((7,)),
            dma,
            dma((31,)),
        ],
        compiler_params=pltpu.CompilerParams(
            collective_id=0, has_side_effects=True, vmem_limit_bytes=63 * 1024 * 1024
        ),
    )(inputs, cotangent, gate, down_weight, up_weight, mixing, table, left, right)


def halves(a):
    hi = a.astype(BF16)
    return hi, (a - hi.astype(F32)).astype(BF16)


def dot(a, b):
    return jnp.dot(a, b, preferred_element_type=F32)


def product(a, b):
    (ah, al), (bh, bl) = a, b
    lhs = jnp.concatenate([ah, ah, al], axis=1)
    rhs = jnp.concatenate([bh, bl, bh], axis=0)
    return dot(lhs, rhs)


def roots(gt_ref, factors, norms, results, filled, out_ref):
    eye = (
        lax.broadcasted_iota(jnp.int32, (R, R), 0) == lax.broadcasted_iota(jnp.int32, (R, R), 1)
    ).astype(F32)
    scaled = gt_ref[...] * (1.0 / TOKENS)
    gt = scaled.astype(BF16)
    g = jnp.transpose(scaled).astype(BF16)
    news = [
        BETA * factors[0] + (1.0 - BETA) * dot(g, gt),
        BETA * factors[1] + (1.0 - BETA) * dot(gt, g),
    ]
    for i, a in enumerate(news):
        shifted = a + EPS * eye
        norm = jnp.sqrt(jnp.sum(shifted * shifted, keepdims=True))
        m = shifted / norm
        results[i] = lax.rsqrt(jnp.sqrt(norm)) * ((5.0 * eye - m) / 4.0)
        norms[i] = m

    def advance(m, mb):
        e = dot(mb, mb) * (1.0 / 16.0) - m * (10.0 / 16.0)
        eb = e.astype(BF16)
        h = (25.0 / 8.0) * e + dot(eb, eb)
        return (625.0 / 256.0) * m + dot(h.astype(BF16), mb)

    def multiply(x, mb):
        return 1.25 * x - 0.25 * dot(x.astype(BF16), mb)

    for i in range(2):
        norms[i] = advance(norms[i], norms[i].astype(BF16))

    def sweep(step, carry):
        for i in range(2):
            m = norms[i]
            mb = m.astype(BF16)
            results[i] = multiply(results[i], mb)
            norms[i] = advance(m, mb)
        return carry

    lax.fori_loop(0, ITERS - 2, sweep, 0, unroll=True)
    left, right = [multiply(results[i], norms[i].astype(BF16)) for i in range(2)]
    half = dot(jnp.concatenate(halves(left), axis=1), jnp.concatenate([g, g], axis=0))
    done = product(halves(half), halves(right))
    out_ref[...] = jnp.where(filled, done, 0.0)


def shards(
    inputs, cotangent, gate, down_weight, up_weight, mixing, owner_table, left_factor, right_factor
):
    table = owner_table.reshape(-1)
    return reduced_block(
        inputs, cotangent, gate.reshape(1, -1), down_weight, up_weight, mixing, table,
        left_factor, right_factor,
    )


def solution(mesh):
    in_specs = (
        P(("rep", "own"), None),
        P(("rep", "own"), None),
        P(("rep", "own")),
        P("rep", None),
        P("rep", None),
        P(),
        P(),
        P("own", None, None),
        P("own", None, None),
    )
    return jax.shard_map(
        shards, mesh=mesh, in_specs=in_specs, out_specs=P("own", None), check_vma=False
    )
```
